256 devices in a mesh: band: 4 (over x), pulse: 16 (over y, z_lo, core), range: 4 (over z_hi).
Axes of the slice: x: 4, y: 4, z: 8 (z_hi: 4, z_lo: 2; z = z_hi * 2 + z_lo), core: 2. Of those that a mesh axis runs over, the one named last changes fastest.
Arguments:
- echoes: bfloat16 [4, 2, 8192, 4096], P('band', None, 'pulse', 'range'), may hold values from -6 to 6
- range_phase: float32 [4, 4096], P('band'), may hold values from -3.140625 to 3.140625
- pulse_shift: int32 [4, 8192], P('band', ('pulse', 'range')), may hold values from -64 to 64
- bin_offset: int32 [4], replicated, may hold values from 0 to 1024, as said below
- doppler_phase: float32 [8192], replicated, may hold values from -3.140625 to 3.140625
Outputs:
- focused: bfloat16 [12288, 2, 8192], P(('band', 'pulse', 'range'))
The draws below stay inside these ranges and needn't reach their ends.
Inputs may be any that keep to these rules, and one draw needn't show every extreme that they name: Band b's spectrum begins at combined bin b * 3072 - 2 * 512 + bin_offset[b]. In every draw some band other than the last has offset 2 * 512 and the band after it has offset 0.
All inputs are finite; a program needn't handle non-finite values.
Results may differ from the reference program's by a relative error of at most 0.0054.
Values may be sent and summed in bfloat16 or wider, within the bound.
No kernel may reach another device: no remote copies, remote signals or barrier semaphores. Data moves between devices by JAX's collectives and lax.ppermute only.
A program may use at most 64 MiB of HBM per device.

```python
import math
import jax
import jax.numpy as jnp
from jax import lax

PULSES = 8192
CELLS = 4096
MARGIN = 512
SHIFT_MAX = 64
BANDS = 4
OWNED = 3072
COMBINED = 12288


def draw_bin_offset(key, part):
    key_draw, key_pick = jax.random.split(jax.random.fold_in(key, 17))
    offsets = jax.random.randint(key_draw, (BANDS,), 0, 2 * MARGIN + 1)
    chosen = jax.random.randint(key_pick, (), 0, BANDS - 1)
    position = jnp.arange(BANDS)
    offsets = jnp.where(position == chosen, 2 * MARGIN, offsets)
    offsets = jnp.where(position == chosen + 1, 0, offsets)
    return offsets.astype(jnp.int32)


def place_ends(entries, key, least, largest):
    shape = entries.shape
    place = [jax.random.randint(jax.random.fold_in(key, axis), (), 0, shape[axis]) for axis in range(len(shape))]
    entries = entries.at[tuple(place)].set(least)
    longest = shape.index(max(shape))
    place[longest] = (place[longest] + 1) % shape[longest]
    return entries.at[tuple(place)].set(largest)


def steps_of(stream_key, shape, pieces, least, high):
    def one(dim, blocks):
        draws = jax.random.uniform(jax.random.fold_in(jax.random.fold_in(stream_key, 6), dim), (blocks,), jnp.float32, least / len(pieces), high / len(pieces))
        return jnp.repeat(jnp.exp(draws), shape[dim] // blocks).reshape((-1,) + (1,) * (len(shape) - dim - 1))

    gain = one(*pieces[0])
    for cut in pieces[1:]:
        gain = gain * one(*cut)
    return gain


def bell_draw(stream_key, extent, scale, reach, shards=(), held_as=jnp.bfloat16):
    factor_of = steps_of(stream_key, extent, shards, -0.22, 0.18) if shards else 1.0
    result = jax.random.normal(stream_key, extent, jnp.float32) * scale * factor_of
    return jnp.minimum(jnp.maximum(result, -reach), reach).astype(held_as)


def setup_inputs(seed: int = 0) -> dict:
    key_list = jax.random.split(jax.random.key(seed), 6)
    echoes = bell_draw(key_list[0], (BANDS, 2, PULSES, CELLS), 1.0, 6.0, ((0, 4), (2, 16), (3, 4)))
    range_phase = jnp.clip(jax.random.uniform(key_list[1], (BANDS, CELLS), jnp.float32, -3.140625, 3.140625), -3.140625, 3.140625)
    pulse_shift = place_ends(jax.random.randint(key_list[2], (BANDS, PULSES), -SHIFT_MAX, SHIFT_MAX + 1), jax.random.fold_in(key_list[2], 1), -SHIFT_MAX, SHIFT_MAX).astype(jnp.int32)
    bin_offset = draw_bin_offset(jax.random.fold_in(key_list[5], 71), 0)
    doppler_phase = jnp.clip(jax.random.uniform(key_list[4], (PULSES,), jnp.float32, -3.140625, 3.140625), -3.140625, 3.140625)
    return dict(echoes=echoes, range_phase=range_phase, pulse_shift=pulse_shift, bin_offset=bin_offset, doppler_phase=doppler_phase)


def rotate(values, angles):
    return values * lax.complex(jnp.cos(angles), jnp.sin(angles))


def round_half(values):
    return lax.optimization_barrier(values.astype(jnp.bfloat16)).astype(jnp.float32)


def reference(echoes, range_phase, pulse_shift, bin_offset, doppler_phase):
    pulse_block = math.gcd(PULSES, 512)
    bin_block = math.gcd(COMBINED, 256)
    cell_index = jnp.arange(CELLS, dtype=jnp.int32)

    def range_section(block_id):
        begin_at = (block_id * pulse_block).astype(jnp.int32)
        samples = lax.dynamic_slice_in_dim(echoes, begin_at, pulse_block, 2).astype(jnp.float32)
        shifts = lax.dynamic_slice_in_dim(pulse_shift, begin_at, pulse_block, 1)
        spectrum = jnp.fft.fft(lax.complex(samples[:, 0], samples[:, 1]), axis=-1, norm="ortho")
        spectrum = rotate(spectrum, range_phase[:, None, :])
        ramp = jnp.mod(cell_index[None, None, :] * shifts[:, :, None], CELLS).astype(jnp.float32) * (-2.0 * math.pi / CELLS)
        spectrum = rotate(spectrum, ramp)
        halves = jnp.stack((round_half(jnp.real(spectrum)), round_half(jnp.imag(spectrum))), axis=1)
        frame_sum = jnp.zeros((2, pulse_block, COMBINED + 4 * MARGIN), jnp.float32)
        anchor_zero = jnp.zeros((), jnp.int32)
        for band_id in range(BANDS):
            placed_at = (band_id * OWNED + bin_offset[band_id]).astype(jnp.int32)
            current = lax.dynamic_slice(frame_sum, (anchor_zero, anchor_zero, placed_at), (2, pulse_block, CELLS))
            frame_sum = lax.dynamic_update_slice(frame_sum, current + halves[band_id], (anchor_zero, anchor_zero, placed_at))
        return frame_sum[:, :, 2 * MARGIN: 2 * MARGIN + COMBINED].astype(jnp.bfloat16)

    blocks = lax.map(range_section, jnp.arange(PULSES // pulse_block, dtype=jnp.int32))
    stitched = jnp.transpose(blocks, (3, 1, 0, 2)).reshape(COMBINED, 2, PULSES)

    def azimuth_section(block_id):
        begin_at = (block_id * bin_block).astype(jnp.int32)
        samples = lax.dynamic_slice_in_dim(stitched, begin_at, bin_block, 0).astype(jnp.float32)
        doppler = jnp.fft.fft(lax.complex(samples[:, 0], samples[:, 1]), axis=-1, norm="ortho")
        doppler = rotate(doppler, doppler_phase[None, :])
        focused_block = jnp.fft.ifft(doppler, axis=-1, norm="ortho")
        return jnp.stack((jnp.real(focused_block), jnp.imag(focused_block)), axis=1).astype(jnp.bfloat16)

    focused = lax.map(azimuth_section, jnp.arange(COMBINED // bin_block, dtype=jnp.int32))
    return focused.reshape(COMBINED, 2, PULSES)
```

```python
import functools
import math

import jax
import jax.numpy as jnp
import ml_dtypes
import numpy as np
from jax import lax
from jax.experimental import pallas as pl
from jax.experimental.pallas import tpu as pltpu
from jax.sharding import PartitionSpec as P

MARGIN = 512
LANES = 128
F32 = jnp.float32
BF16 = jnp.bfloat16


def split_const(table):
    high = table.astype(ml_dtypes.bfloat16)
    low = (table - high.astype(np.float64)).astype(ml_dtypes.bfloat16)
    return high, low


def unit_roots(rows, cols, modulus, sign):
    product = np.outer(np.arange(rows), np.arange(cols)) % modulus
    angle = sign * 2.0 * np.pi * product / modulus
    return np.cos(angle), np.sin(angle)


def split_value(value):
    high = value.astype(BF16)
    low = (value - high.astype(F32)).astype(BF16)
    return high, low


def dot_f32(lhs, rhs, contract):
    return lax.dot_general(lhs, rhs, (contract, ((), ())), preferred_element_type=F32)


def dot_three(lhs, rhs, contract):
    return (
        dot_f32(lhs[0], rhs[0], contract)
        + dot_f32(lhs[0], rhs[1], contract)
        + dot_f32(lhs[1], rhs[0], contract)
    )


def complex_mul(a, b):
    return a[0] * b[0] - a[1] * b[1], a[0] * b[1] + a[1] * b[0]


def by_constant(a, angle):
    cos = math.cos(angle)
    sin = math.sin(angle)
    quarter = angle / (math.pi / 2)
    if abs(quarter - round(quarter)) < 1e-9:
        turn = int(round(quarter)) % 4
        if turn == 0:
            return a
        if turn == 1:
            return -a[1], a[0]
        if turn == 2:
            return -a[0], -a[1]
        return a[1], -a[0]
    if abs(abs(cos) - abs(sin)) < 1e-9:
        half = math.sqrt(0.5)
        plus = (a[0] + a[1]) * half
        minus = (a[0] - a[1]) * half
        if cos > 0 and sin > 0:
            return minus, plus
        if cos < 0 and sin > 0:
            return -plus, minus
        if cos < 0 and sin < 0:
            return -minus, -plus
        return plus, -minus
    return a[0] * cos - a[1] * sin, a[0] * sin + a[1] * cos


def small_dft(values, sign):
    count = len(values)
    if count == 1:
        return values
    even = small_dft(values[0::2], sign)
    odd = small_dft(values[1::2], sign)
    first = []
    second = []
    for i in range(count // 2):
        turned = by_constant(odd[i], sign * 2.0 * math.pi * i / count)
        first.append((even[i][0] + turned[0], even[i][1] + turned[1]))
        second.append((even[i][0] - turned[0], even[i][1] - turned[1]))
    return first + second


def range_kernel(outer, sub, rows, shift_ref, echo_ref, twist_ref, cos_ref, sin_ref,
                 high_ref, low_ref, out_ref, stage_ref, mid_ref):
    step = pl.program_id(0)
    sources = echo_ref.shape[0]
    inner = outer // sources
    group = 16

    @pl.when(step == 0)
    def _():
        def block(t, carry):
            at = pl.multiple_of(t * group, group)
            for n in range(inner):
                lanes = slice(n * LANES, (n + 1) * LANES)
                values = []
                for z in range(sources):
                    values.append((
                        echo_ref[z, 0, pl.ds(at, group), lanes].astype(F32),
                        echo_ref[z, 1, pl.ds(at, group), lanes].astype(F32),
                    ))
                for q, value in enumerate(small_dft(values, -1.0)):
                    value = by_constant(value, -2.0 * math.pi * n * q / outer)
                    mid_ref[q, n, 0] = value[0]
                    mid_ref[q, n, 1] = value[1]
            for q in range(sources):
                values = [(mid_ref[q, n, 0], mid_ref[q, n, 1]) for n in range(inner)]
                for m, value in enumerate(small_dft(values, -1.0)):
                    stage_ref[q + sources * m, 0, pl.ds(at, group), :] = value[0]
                    stage_ref[q + sources * m, 1, pl.ds(at, group), :] = value[1]
            return carry

        lax.fori_loop(0, rows // group, block, 0)

    shift = shift_ref[0]
    per_step = cos_ref.shape[0]
    for i in range(per_step):
        real_rows = []
        imag_rows = []
        for h in range(sub):
            bin_low = (step * per_step + i) * sub + h
            source = lax.rem(bin_low - shift + 2 * outer, outer)
            twist = (twist_ref[0, pl.ds(bin_low, 1), :], twist_ref[1, pl.ds(bin_low, 1), :])
            value = complex_mul((stage_ref[source, 0], stage_ref[source, 1]), twist)
            real_rows.append(value[0])
            imag_rows.append(value[1])
        real = jnp.concatenate(real_rows, axis=0) if sub > 1 else real_rows[0]
        imag = jnp.concatenate(imag_rows, axis=0) if sub > 1 else imag_rows[0]
        data = split_value(jnp.concatenate((real, imag), axis=1))
        product = dot_three((high_ref[...], low_ref[...]), data, ((1,), (1,)))
        half = product.shape[0] // 2
        value = product[:half] * cos_ref[i] + product[half:] * sin_ref[i]
        out_ref[i] = value.astype(BF16)


def range_tables():
    cos, sin = unit_roots(LANES, LANES, LANES, -1.0)
    plain = np.zeros((LANES, 2, 2, LANES))
    turned = np.zeros((LANES, 2, 2, LANES))
    plain[:, 0, 0], plain[:, 0, 1] = cos, -sin
    plain[:, 1, 0], plain[:, 1, 1] = sin, cos
    turned[:, 0] = -plain[:, 1]
    turned[:, 1] = plain[:, 0]
    return split_const(np.concatenate((plain, turned)).reshape(4 * LANES, 2 * LANES))


def range_stage(received, twist, cos, sin, shift, outer, sub):
    rows = received.shape[2]
    steps = cos.shape[0]
    per_step = 2
    high, low = range_tables()
    kernel = functools.partial(range_kernel, outer, sub, rows)
    whole = lambda shape: pl.BlockSpec(shape, lambda i: (0,) * len(shape))
    return pl.pallas_call(
        kernel,
        grid=(steps // per_step,),
        in_specs=[
            pl.BlockSpec(memory_space=pltpu.SMEM),
            whole(received.shape),
            whole(twist.shape),
            pl.BlockSpec((per_step, 2 * LANES, LANES), lambda i: (i, 0, 0)),
            pl.BlockSpec((per_step, 2 * LANES, LANES), lambda i: (i, 0, 0)),
            whole(high.shape),
            whole(low.shape),
        ],
        out_specs=pl.BlockSpec((per_step, 2 * LANES, LANES), lambda i: (i, 0, 0)),
        out_shape=jax.ShapeDtypeStruct((steps, 2 * LANES, LANES), BF16),
        scratch_shapes=[
            pltpu.VMEM((outer, 2, rows, LANES), F32),
            pltpu.VMEM((received.shape[0], outer // received.shape[0], 2, 16, LANES), F32),
        ],
        compiler_params=pltpu.CompilerParams(
            dimension_semantics=("arbitrary",), vmem_limit_bytes=48 * 1024 * 1024),
        name="range_stage",
    )(shift, received, twist, cos, sin, jnp.asarray(high), jnp.asarray(low))


def azimuth_kernel(outer, first_ref, fore_ref, twist_ref, filter_ref, back_ref, last_ref,
                   data_ref, out_ref):
    count = data_ref.shape[0]
    twist = (twist_ref[0], twist_ref[1])
    twist_back = (twist_ref[0], -twist_ref[1])
    turn = (filter_ref[0], filter_ref[1])
    left = ((1,), (0,))
    rows = []
    for c in range(count):
        spread = dot_f32(first_ref[0], data_ref[c], left) + dot_f32(first_ref[1], data_ref[c], left)
        value = complex_mul((spread[:outer], spread[outer:]), twist)
        rows.append(jnp.concatenate(value, axis=1))
    stacked = split_value(jnp.concatenate(rows, axis=0))
    doppler = dot_three(stacked, (fore_ref[0], fore_ref[1]), left)
    rows = []
    for c in range(count):
        part = doppler[c * outer:(c + 1) * outer]
        rows.append(jnp.concatenate(complex_mul((part[:, :LANES], part[:, LANES:]), turn), axis=1))
    stacked = split_value(jnp.concatenate(rows, axis=0))
    image = dot_three(stacked, (back_ref[0], back_ref[1]), left)
    for c in range(count):
        part = image[c * outer:(c + 1) * outer]
        value = complex_mul((part[:, :LANES], part[:, LANES:]), twist_back)
        value = split_value(jnp.concatenate(value, axis=0))
        out_ref[c] = dot_three((last_ref[0], last_ref[1]), value, left).astype(BF16)


def azimuth_tables(outer):
    cos, sin = unit_roots(outer, outer, outer, -1.0)
    first = np.zeros((2, outer, outer, 2))
    first[0, :, :, 0], first[0, :, :, 1] = cos, -sin
    first[1, :, :, 0], first[1, :, :, 1] = sin, cos
    last = np.zeros((outer, 2, 2, outer))
    last[:, 0, 0], last[:, 0, 1] = cos, sin
    last[:, 1, 0], last[:, 1, 1] = -sin, cos
    cos, sin = unit_roots(LANES, LANES, LANES, -1.0)
    fore = np.zeros((2, LANES, 2, LANES))
    fore[0, :, 0], fore[0, :, 1] = cos, sin
    fore[1, :, 0], fore[1, :, 1] = -sin, cos
    back = np.zeros((2, LANES, 2, LANES))
    back[0, :, 0], back[0, :, 1] = cos, -sin
    back[1, :, 0], back[1, :, 1] = sin, cos
    pair = lambda table, shape: np.stack(split_const(table.reshape(shape)))
    twist = np.stack(unit_roots(outer, LANES, outer * LANES, -1.0)).astype(np.float32)
    square = (2 * LANES, 2 * LANES)
    side = (2 * outer, 2 * outer)
    return pair(first, side), pair(fore, square), twist, pair(back, square), pair(last, side)


def azimuth_stage(data, turn, outer):
    count = data.shape[0]
    block = 8
    first, fore, twist, back, last = azimuth_tables(outer)
    whole = lambda shape: pl.BlockSpec(shape, lambda i: (0,) * len(shape))
    tile = pl.BlockSpec((block,) + data.shape[1:], lambda i: (i, 0, 0))
    constants = (first, fore, twist)
    return pl.pallas_call(
        functools.partial(azimuth_kernel, outer),
        grid=(count // block,),
        in_specs=[whole(first.shape), whole(fore.shape), whole(twist.shape), whole(turn.shape),
                  whole(back.shape), whole(last.shape), tile],
        out_specs=tile,
        out_shape=jax.ShapeDtypeStruct(data.shape, BF16),
        compiler_params=pltpu.CompilerParams(
            dimension_semantics=("arbitrary",), vmem_limit_bytes=48 * 1024 * 1024),
        name="azimuth_stage",
    )(jnp.asarray(first), jnp.asarray(fore), jnp.asarray(twist), turn, jnp.asarray(back),
      jnp.asarray(last), data)


def shifted(block, distance):
    devices = range(lax.axis_size("band"))
    route = [(i - distance, i) for i in devices if i - distance in devices]
    return lax.ppermute(block, "band", route)


def body(echoes, range_phase, pulse_shift, bin_offset, doppler_phase):
    range_count = lax.axis_size("range")
    group_size = lax.axis_size("pulse") * range_count
    cells_local = echoes.shape[3]
    cell_count = cells_local * range_count
    n_local = echoes.shape[2] // range_count
    spill_len = 2 * MARGIN
    owned_bins = cell_count - spill_len
    bins_local = owned_bins // group_size
    outer = cell_count // LANES
    sub = 1

    band = lax.axis_index("band")
    bands = bin_offset.shape[0]
    order = jnp.arange(bands, dtype=jnp.int32)
    offset_of = lambda index: jnp.sum(jnp.where(order == index, bin_offset, 0))
    offset = offset_of(band)
    below = offset_of(band - 1)
    above = offset_of(band + 1)
    shift = offset - spill_len

    rows_in = echoes[0].reshape(2, range_count, n_local, cells_local)
    rows_in = jnp.transpose(rows_in, (1, 0, 2, 3))
    received = lax.all_to_all(rows_in, "range", split_axis=0, concat_axis=0, tiled=True)

    low = jnp.arange(outer, dtype=jnp.int32)
    lane = jnp.arange(LANES, dtype=jnp.int32)
    angle = jnp.mod((low[:, None] - shift) * lane[None, :], cell_count).astype(F32) * (
        -2.0 * math.pi / cell_count)
    twist = jnp.stack((jnp.cos(angle), jnp.sin(angle)))
    phase = jnp.concatenate((range_phase[0], range_phase[0]))
    phase = lax.dynamic_slice_in_dim(phase, spill_len - offset, cell_count, 0)
    phase = jnp.transpose(phase.reshape(LANES, outer))
    index = jnp.mod(low[:, None] + outer * lane[None, :] - shift, cell_count)
    ramp = jnp.mod(index[:, :, None] * pulse_shift[0][None, None, :], cell_count).astype(F32) * (
        -2.0 * math.pi / cell_count)
    theta = phase[:, :, None] + ramp
    double = lambda value: jnp.broadcast_to(
        value[:, :, None, :], (outer, LANES, 2, LANES)).reshape(outer, 2 * LANES, LANES)
    scale = 1.0 / math.sqrt(cell_count)
    cos = double(jnp.cos(theta) * scale)
    sin = double(jnp.sin(theta) * scale)

    spectrum = range_stage(received, twist, cos, sin, shift.reshape(1), outer, sub)
    spectrum = jnp.transpose(spectrum.reshape(outer, LANES, 2, LANES), (1, 0, 2, 3))
    spectrum = spectrum.reshape(cell_count, 2, LANES)
    spill = spectrum[owned_bins:]
    from_below = shifted(spill, 1)
    from_above = shifted(spill, -1)
    row = jnp.arange(spill_len, dtype=jnp.int32)[:, None, None]
    add_low = jnp.where(row < below, from_below.astype(F32), 0.0)
    add_high = jnp.where(row >= above, from_above.astype(F32), 0.0)
    first = spectrum[:spill_len].astype(F32) + add_low
    middle = spectrum[spill_len:owned_bins - spill_len]
    final = spectrum[owned_bins - spill_len:owned_bins].astype(F32) + add_high
    stitched = jnp.concatenate((first.astype(BF16), middle, final.astype(BF16)))
    blocks = stitched.reshape(group_size, bins_local, 2, LANES)
    samples = lax.all_to_all(blocks, ("pulse", "range"), split_axis=0, concat_axis=0, tiled=True)

    samples = jnp.transpose(samples, (1, 0, 2, 3)).reshape(bins_local, 2 * group_size, LANES)
    doppler = jnp.transpose(doppler_phase.reshape(LANES, group_size))
    factor = 1.0 / doppler_phase.shape[0]
    turn = jnp.stack((jnp.cos(doppler) * factor, jnp.sin(doppler) * factor))
    image = azimuth_stage(samples, turn, group_size)
    image = jnp.transpose(image.reshape(bins_local, group_size, 2, LANES), (0, 2, 1, 3))
    return image.reshape(bins_local, 2, group_size * LANES)


def solution(mesh):
    in_specs = (
        P("band", None, "pulse", "range"),
        P("band", None),
        P("band", ("pulse", "range")),
        P(),
        P(),
    )
    out_specs = P(("band", "pulse", "range"), None, None)
    return jax.shard_map(body, mesh=mesh, in_specs=in_specs, out_specs=out_specs, check_vma=False)
```

```python
import functools
import math

import jax
import jax.numpy as jnp
import ml_dtypes
import numpy as np
from jax import lax
from jax.experimental import pallas as pl
from jax.experimental.pallas import tpu as pltpu
from jax.sharding import PartitionSpec as P


MARGIN = 512
LANES = 128
CHUNKS = 2
F32 = jnp.float32
BF16 = jnp.bfloat16


def split_const(table):
    high = table.astype(ml_dtypes.bfloat16)
    low = (table - high.astype(np.float64)).astype(ml_dtypes.bfloat16)
    return high, low


def unit_roots(rows, cols, modulus, sign):
    product = np.outer(np.arange(rows), np.arange(cols)) % modulus
    angle = sign * 2.0 * np.pi * product / modulus
    return np.cos(angle), np.sin(angle)


def dot_f32(lhs, rhs, contract):
    return lax.dot_general(lhs, rhs, (contract, ((), ())), preferred_element_type=F32)


def complex_mul(a, b):
    return a[0] * b[0] - a[1] * b[1], a[0] * b[1] + a[1] * b[0]


def by_constant(a, angle):
    cos = math.cos(angle)
    sin = math.sin(angle)
    quarter = angle / (math.pi / 2)
    if abs(quarter - round(quarter)) < 1e-9:
        turn = int(round(quarter)) % 4
        if turn == 0:
            return a
        if turn == 1:
            return -a[1], a[0]
        if turn == 2:
            return -a[0], -a[1]
        return a[1], -a[0]
    if abs(abs(cos) - abs(sin)) < 1e-9:
        half = math.sqrt(0.5)
        plus = (a[0] + a[1]) * half
        minus = (a[0] - a[1]) * half
        if cos > 0 and sin > 0:
            return minus, plus
        if cos < 0 and sin > 0:
            return -plus, minus
        if cos < 0 and sin < 0:
            return -minus, -plus
        return plus, -minus
    return a[0] * cos - a[1] * sin, a[0] * sin + a[1] * cos


def small_dft(values, sign):
    count = len(values)
    if count == 1:
        return values
    even = small_dft(values[0::2], sign)
    odd = small_dft(values[1::2], sign)
    first = []
    second = []
    for i in range(count // 2):
        turned = by_constant(odd[i], sign * 2.0 * math.pi * i / count)
        first.append((even[i][0] + turned[0], even[i][1] + turned[1]))
        second.append((even[i][0] - turned[0], even[i][1] - turned[1]))
    return first + second


def range_kernel(outer, sub, sources, shift_ref, *refs):
    echo_refs = refs[:sources]
    (twist_ref, near_ref, far_ref, phase_ref, table_ref, _, own_ref, spill_ref,
     stage_ref, mid_ref, order_ref) = refs[sources:]
    step = pl.program_id(0)
    rows = echo_refs[0].shape[1]
    inner = outer // sources
    group = 16

    @pl.when(step == 0)
    def _():
        def block(t, carry):
            at = pl.multiple_of(t * group, group)
            for n in range(inner):
                lanes = slice(n * LANES, (n + 1) * LANES)
                values = []
                for echo_ref in echo_refs:
                    values.append((
                        echo_ref[0, pl.ds(at, group), lanes].astype(F32),
                        echo_ref[1, pl.ds(at, group), lanes].astype(F32),
                    ))
                for q, value in enumerate(small_dft(values, -1.0)):
                    value = by_constant(value, -2.0 * math.pi * n * q / outer)
                    mid_ref[q, n, 0] = value[0]
                    mid_ref[q, n, 1] = value[1]
            for q in range(sources):
                values = [(mid_ref[q, n, 0], mid_ref[q, n, 1]) for n in range(inner)]
                for m, value in enumerate(small_dft(values, -1.0)):
                    stage_ref[q + sources * m, 0, pl.ds(at, group), :] = value[0]
                    stage_ref[q + sources * m, 1, pl.ds(at, group), :] = value[1]
            return carry

        lax.fori_loop(0, rows // group, block, 0)

    shift = shift_ref[0]
    per_step = phase_ref.shape[1]
    parts = []
    for i in range(per_step * sub):
        bin_low = step * per_step * sub + i
        source = lax.rem(bin_low - shift + 2 * outer, outer)
        twist = (twist_ref[0, pl.ds(bin_low, 1), :], twist_ref[1, pl.ds(bin_low, 1), :])
        value = complex_mul((stage_ref[source, 0], stage_ref[source, 1]), twist)
        parts.append(jnp.concatenate(value, axis=1).astype(BF16))
    data = jnp.concatenate(parts, axis=0)
    across = ((1,), (1,))
    product = dot_f32(table_ref[0], data, across) + dot_f32(table_ref[1], data, across)
    steps = outer // sub
    pitch = order_ref.shape[0] // LANES
    far = (far_ref[0], far_ref[1])
    for i in range(per_step):
        lanes = slice(i * LANES, (i + 1) * LANES)
        at = step * per_step + i
        near = (near_ref[0, pl.ds(at, 1), :], near_ref[1, pl.ds(at, 1), :])
        turn = complex_mul(complex_mul(far, near), (phase_ref[0, i], phase_ref[1, i]))
        real, imag = complex_mul((product[:LANES, lanes], product[LANES:, lanes]), turn)
        order_ref[pl.ds(2 * at, LANES, stride=pitch), :] = real
        order_ref[pl.ds(2 * at + 1, LANES, stride=pitch), :] = imag

    @pl.when(step == pl.num_programs(0) - 1)
    def _():
        width = 2 * steps
        owned = own_ref.shape[0] // width
        for n in range(LANES):
            value = order_ref[n * pitch:n * pitch + width, :].astype(BF16)
            if n < owned:
                own_ref[n * width:(n + 1) * width, :] = value
            else:
                spill_ref[(n - owned) * width:(n - owned + 1) * width, :] = value


def range_tables():
    cos, sin = unit_roots(LANES, LANES, LANES, -1.0)
    table = np.zeros((2, LANES, 2, LANES))
    table[0, :, 0], table[0, :, 1] = cos, -sin
    table[1, :, 0], table[1, :, 1] = sin, cos
    return np.stack(split_const(table.reshape(2 * LANES, 2 * LANES)))


def range_stage(received, twist, near, far, phase, gate, shift, outer, sub, owned_rows):
    sources = len(received)
    rows = received[0].shape[1]
    steps = outer // sub
    per_step = 2
    pitch = 2 * steps + 8
    table = range_tables()
    whole = lambda shape: pl.BlockSpec(shape, lambda i: (0,) * len(shape))
    return pl.pallas_call(
        functools.partial(range_kernel, outer, sub, sources),
        grid=(steps // per_step,),
        in_specs=[
            pl.BlockSpec(memory_space=pltpu.SMEM),
            *[whole(block.shape) for block in received],
            whole(twist.shape),
            whole(near.shape),
            whole(far.shape),
            pl.BlockSpec((2, per_step, LANES, LANES), lambda i: (0, i, 0, 0)),
            whole(table.shape),
            pl.BlockSpec(memory_space=pl.ANY),
        ],
        out_specs=[whole((2 * owned_rows, LANES)),
                   whole((2 * steps * LANES - 2 * owned_rows, LANES))],
        out_shape=[jax.ShapeDtypeStruct((2 * owned_rows, LANES), BF16),
                   jax.ShapeDtypeStruct((2 * steps * LANES - 2 * owned_rows, LANES), BF16)],
        scratch_shapes=[
            pltpu.VMEM((outer, 2, rows, LANES), F32),
            pltpu.VMEM((sources, outer // sources, 2, 16, LANES), F32),
            pltpu.VMEM((LANES * pitch, LANES), F32),
        ],
        compiler_params=pltpu.CompilerParams(
            dimension_semantics=("arbitrary",), vmem_limit_bytes=48 * 1024 * 1024),
        name="range_stage",
    )(shift, *received, twist, near, far, phase, jnp.asarray(table), gate)


def stitch_kernel(sub, limits_ref, own_ref, low_ref, high_ref, out_ref):
    side = pl.program_id(0)
    shape = own_ref.shape
    row = lax.broadcasted_iota(jnp.int32, shape, 0) // 2
    lane = lax.broadcasted_iota(jnp.int32, shape, 1)
    index = row * sub + lane // (LANES // sub)

    @pl.when(side == 0)
    def _():
        added = jnp.where(index < limits_ref[0], low_ref[...].astype(F32), 0.0)
        out_ref[...] = (own_ref[...].astype(F32) + added).astype(BF16)

    @pl.when(side == 1)
    def _():
        added = jnp.where(index >= limits_ref[1], high_ref[...].astype(F32), 0.0)
        out_ref[...] = (own_ref[...].astype(F32) + added).astype(BF16)


def stitch(own, from_below, from_above, limits, sub):
    height = from_below.shape[0]
    last = own.shape[0] // height - 1
    side = pl.BlockSpec((height, LANES), lambda i: (i * last, 0))
    whole = pl.BlockSpec((height, LANES), lambda i: (0, 0))
    return pl.pallas_call(
        functools.partial(stitch_kernel, sub),
        grid=(2,),
        in_specs=[pl.BlockSpec(memory_space=pltpu.SMEM), side, whole, whole],
        out_specs=side,
        out_shape=jax.ShapeDtypeStruct(own.shape, BF16),
        input_output_aliases={1: 0},
        compiler_params=pltpu.CompilerParams(dimension_semantics=("arbitrary",)),
        name="stitch",
    )(limits, own, from_below, from_above)


def azimuth_kernel(outer, first_ref, fore_ref, twist_ref, filter_ref, back_ref, last_ref, *refs):
    data_refs = refs[:-1]
    out_ref = refs[-1]
    chunks = len(data_refs)
    width = LANES // chunks
    count = data_refs[0].shape[0]
    twist = (twist_ref[0], twist_ref[1])
    twist_back = (twist_ref[0], -twist_ref[1])
    turn = (filter_ref[0], filter_ref[1])
    left = ((1,), (0,))
    two = lambda lhs, rhs: dot_f32(lhs[0], rhs, left) + dot_f32(lhs[1], rhs, left)
    rows = []
    for c in range(count):
        data = [ref[c] for ref in data_refs]
        spread = two((first_ref[0], first_ref[1]), jnp.concatenate(data, axis=1))
        for h in range(chunks):
            pieces = [spread[:, q * LANES + h * width:q * LANES + (h + 1) * width]
                      for q in range(chunks)]
            joined = jnp.concatenate(pieces, axis=1)
            value = complex_mul((joined[:outer], joined[outer:]), twist)
            rows.append(jnp.concatenate(value, axis=1).astype(BF16))
    total = count * chunks
    stacked = jnp.concatenate(rows, axis=0)
    doppler = dot_f32(stacked, fore_ref[0], left) + dot_f32(stacked, fore_ref[1], left)
    rows = []
    for c in range(total):
        part = doppler[c * outer:(c + 1) * outer]
        value = complex_mul((part[:, :LANES], part[:, LANES:]), turn)
        rows.append(jnp.concatenate(value, axis=1).astype(BF16))
    stacked = jnp.concatenate(rows, axis=0)
    image = dot_f32(stacked, back_ref[0], left) + dot_f32(stacked, back_ref[1], left)
    for c in range(0, total, 2):
        values = []
        for d in range(2):
            part = image[(c + d) * outer:(c + d + 1) * outer]
            value = complex_mul((part[:, :LANES], part[:, LANES:]), twist_back)
            values.append(jnp.concatenate(value, axis=0).astype(BF16))
        value = two((last_ref[0], last_ref[1]), jnp.concatenate(values, axis=1)).astype(BF16)
        out_ref[c] = value[:, :LANES]
        out_ref[c + 1] = value[:, LANES:]


def azimuth_tables(outer):
    cos, sin = unit_roots(outer, outer, outer, -1.0)
    first = np.zeros((2, outer, outer, 2))
    first[0, :, :, 0], first[0, :, :, 1] = cos, -sin
    first[1, :, :, 0], first[1, :, :, 1] = sin, cos
    last = np.zeros((outer, 2, 2, outer))
    last[:, 0, 0], last[:, 0, 1] = cos, sin
    last[:, 1, 0], last[:, 1, 1] = -sin, cos
    cos, sin = unit_roots(LANES, LANES, LANES, -1.0)
    fore = np.zeros((2, LANES, 2, LANES))
    fore[0, :, 0], fore[0, :, 1] = cos, sin
    fore[1, :, 0], fore[1, :, 1] = -sin, cos
    back = np.zeros((2, LANES, 2, LANES))
    back[0, :, 0], back[0, :, 1] = cos, -sin
    back[1, :, 0], back[1, :, 1] = sin, cos
    pair = lambda table, shape: np.stack(split_const(table.reshape(shape)))
    twist = np.stack(unit_roots(outer, LANES, outer * LANES, -1.0)).astype(np.float32)
    square = (2 * LANES, 2 * LANES)
    side = (2 * outer, 2 * outer)
    return pair(first, side), pair(fore, square), twist, pair(back, square), pair(last, side)


def azimuth_stage(data, turn, outer):
    chunks = len(data)
    count = data[0].shape[0]
    block = 8 // chunks
    first, fore, twist, back, last = azimuth_tables(outer)
    whole = lambda shape: pl.BlockSpec(shape, lambda i: (0,) * len(shape))
    tile = pl.BlockSpec((block,) + data[0].shape[1:], lambda i: (i, 0, 0))
    out_shape = (count * chunks,) + data[0].shape[1:]
    return pl.pallas_call(
        functools.partial(azimuth_kernel, outer),
        grid=(count // block,),
        in_specs=[whole(first.shape), whole(fore.shape), whole(twist.shape), whole(turn.shape),
                  whole(back.shape), whole(last.shape)] + [tile] * chunks,
        out_specs=pl.BlockSpec((block * chunks,) + out_shape[1:], lambda i: (i, 0, 0)),
        out_shape=jax.ShapeDtypeStruct(out_shape, BF16),
        compiler_params=pltpu.CompilerParams(
            dimension_semantics=("arbitrary",), vmem_limit_bytes=48 * 1024 * 1024),
        name="azimuth_stage",
    )(jnp.asarray(first), jnp.asarray(fore), jnp.asarray(twist), turn, jnp.asarray(back),
      jnp.asarray(last), *data)


def shifted(block, distance):
    devices = range(lax.axis_size("band"))
    route = [(i - distance, i) for i in devices if i - distance in devices]
    return lax.ppermute(block, "band", route)


def body(echoes, range_phase, pulse_shift, bin_offset, doppler_phase):
    range_count = lax.axis_size("range")
    group_size = lax.axis_size("pulse") * range_count
    cells_local = echoes.shape[3]
    cell_count = cells_local * range_count
    n_local = echoes.shape[2] // range_count
    spill_len = 2 * MARGIN
    owned_bins = cell_count - spill_len
    bins_local = owned_bins // group_size
    outer = cell_count // LANES
    sub = CHUNKS
    piece = n_local // sub
    steps = outer // sub
    owned_rows = owned_bins // sub

    band = lax.axis_index("band")
    bands = bin_offset.shape[0]
    order = jnp.arange(bands, dtype=jnp.int32)
    offset_of = lambda index: jnp.sum(jnp.where(order == index, bin_offset, 0))
    offset = offset_of(band)
    below = offset_of(band - 1)
    above = offset_of(band + 1)
    shift = offset - spill_len

    place = lax.axis_index("range")
    low = jnp.arange(outer, dtype=jnp.int32)
    lane = jnp.arange(LANES, dtype=jnp.int32)
    phase = jnp.concatenate((range_phase[0], range_phase[0]))
    phase = lax.dynamic_slice_in_dim(phase, spill_len - offset, cell_count, 0)
    phase = jnp.transpose(phase.reshape(LANES, steps, sub), (2, 1, 0))
    scale = 1.0 / math.sqrt(cell_count)
    phase = jnp.stack((jnp.cos(phase) * scale, jnp.sin(phase) * scale))
    cube = (2, steps, LANES, LANES)
    part = lane // piece
    spread = jnp.broadcast_to(phase[:, sub - 1][..., None], cube)
    for h in range(sub - 1):
        spread = jnp.where(part == h, phase[:, h][..., None], spread)
    low_bin = jnp.arange(steps, dtype=jnp.int32)[:, None] * sub + part - shift

    def ramp(product):
        angle = jnp.mod(product, cell_count).astype(F32) * (-2.0 * math.pi / cell_count)
        return jnp.stack((jnp.cos(angle), jnp.sin(angle)))

    doppler = jnp.transpose(doppler_phase.reshape(LANES, group_size))
    factor = 1.0 / doppler_phase.shape[0]
    turn = jnp.stack((jnp.cos(doppler) * factor, jnp.sin(doppler) * factor))

    received = []
    for q in range(sub):
        blocks = []
        for d in range(range_count):
            begin = jnp.mod(place + d, range_count) * n_local + q * piece
            block = lax.dynamic_slice_in_dim(echoes[0], begin, piece, 1)
            if d:
                route = [(i, (i + d) % range_count) for i in range(range_count)]
                block = lax.ppermute(block, "range", route)
            blocks.append(block)
        received.append([blocks[(-z) % range_count] for z in range(range_count)])

    twist = ramp((low[:, None] - shift) * (lane[None, :] + cells_local * place))
    limits = jnp.stack((below, above))
    samples = []
    gate = None
    for q in range(sub):
        shifts = jnp.tile(pulse_shift[0, q * piece:(q + 1) * piece], sub)
        near = ramp(low_bin * shifts)
        far = ramp(outer * lane[:, None] * shifts)
        gate = twist if gate is None else gate
        own, spill = range_stage(received[q], twist, near, far, spread, gate,
                                 shift.reshape(1), outer, sub, owned_rows)
        from_below = shifted(spill, 1)
        from_above = shifted(spill, -1)
        gate = stitch(own, from_below, from_above, limits, sub)
        blocks = gate.reshape(group_size, bins_local // sub, 2, LANES)
        block = lax.all_to_all(
            blocks, ("pulse", "range"), split_axis=0, concat_axis=0, tiled=True)
        samples.append(jnp.transpose(block, (1, 0, 2, 3)).reshape(
            bins_local // sub, 2 * group_size, LANES))

    image = azimuth_stage(samples, turn, group_size)
    image = jnp.transpose(image.reshape(bins_local, group_size, 2, LANES), (0, 2, 1, 3))
    return image.reshape(bins_local, 2, group_size * LANES)


def solution(mesh):
    in_specs = (
        P("band", None, "pulse", "range"),
        P("band", None),
        P("band", ("pulse", "range")),
        P(),
        P(),
    )
    out_specs = P(("band", "pulse", "range"), None, None)
    return jax.shard_map(
        body, mesh=mesh, in_specs=in_specs, out_specs=out_specs, check_vma=False)
```

```python
import functools
import math

import jax
import jax.numpy as jnp
import ml_dtypes
import numpy as np
from jax import lax
from jax.experimental import pallas as pl
from jax.experimental.pallas import tpu as pltpu
from jax.sharding import PartitionSpec as P


MARGIN = 512
LANES = 128
CHUNKS = 2
F32 = jnp.float32
BF16 = jnp.bfloat16


def split_const(table):
    high = table.astype(ml_dtypes.bfloat16)
    low = (table - high.astype(np.float64)).astype(ml_dtypes.bfloat16)
    return high, low


def unit_roots(rows, cols, modulus, sign):
    product = np.outer(np.arange(rows), np.arange(cols)) % modulus
    angle = sign * 2.0 * np.pi * product / modulus
    return np.cos(angle), np.sin(angle)


def dot_f32(lhs, rhs, contract):
    return lax.dot_general(lhs, rhs, (contract, ((), ())), preferred_element_type=F32)


def complex_mul(a, b):
    return a[0] * b[0] - a[1] * b[1], a[0] * b[1] + a[1] * b[0]


def by_constant(a, angle):
    cos = math.cos(angle)
    sin = math.sin(angle)
    quarter = angle / (math.pi / 2)
    if abs(quarter - round(quarter)) < 1e-9:
        turn = int(round(quarter)) % 4
        if turn == 0:
            return a
        if turn == 1:
            return -a[1], a[0]
        if turn == 2:
            return -a[0], -a[1]
        return a[1], -a[0]
    if abs(abs(cos) - abs(sin)) < 1e-9:
        half = math.sqrt(0.5)
        plus = (a[0] + a[1]) * half
        minus = (a[0] - a[1]) * half
        if cos > 0 and sin > 0:
            return minus, plus
        if cos < 0 and sin > 0:
            return -plus, minus
        if cos < 0 and sin < 0:
            return -minus, -plus
        return plus, -minus
    return a[0] * cos - a[1] * sin, a[0] * sin + a[1] * cos


def small_dft(values, sign):
    count = len(values)
    if count == 1:
        return values
    even = small_dft(values[0::2], sign)
    odd = small_dft(values[1::2], sign)
    first = []
    second = []
    for i in range(count // 2):
        turned = by_constant(odd[i], sign * 2.0 * math.pi * i / count)
        first.append((even[i][0] + turned[0], even[i][1] + turned[1]))
        second.append((even[i][0] - turned[0], even[i][1] - turned[1]))
    return first + second


def range_kernel(outer, sub, sources, scalar_ref, mine_ref, *refs):
    echo_refs = (mine_ref,) + refs[:sources - 1]
    (twist_ref, near_ref, far_ref, phase_ref, table_ref, _, own_ref, spill_ref,
     stage_ref, mid_ref, order_ref) = refs[sources - 1:]
    step = pl.program_id(0)
    rows = echo_refs[0].shape[1]
    inner = outer // sources
    group = 16

    @pl.when(step == 0)
    def _():
        def block(t, carry):
            at = pl.multiple_of(t * group, group)
            for n in range(inner):
                lanes = slice(n * LANES, (n + 1) * LANES)
                values = []
                for echo_ref in echo_refs:
                    values.append((
                        echo_ref[0, pl.ds(at, group), lanes].astype(F32),
                        echo_ref[1, pl.ds(at, group), lanes].astype(F32),
                    ))
                for q, value in enumerate(small_dft(values, -1.0)):
                    value = by_constant(value, -2.0 * math.pi * n * q / outer)
                    mid_ref[q, n, 0] = value[0]
                    mid_ref[q, n, 1] = value[1]
            for q in range(sources):
                values = [(mid_ref[q, n, 0], mid_ref[q, n, 1]) for n in range(inner)]
                for m, value in enumerate(small_dft(values, -1.0)):
                    stage_ref[q + sources * m, 0, pl.ds(at, group), :] = value[0]
                    stage_ref[q + sources * m, 1, pl.ds(at, group), :] = value[1]
            return carry

        lax.fori_loop(0, rows // group, block, 0)

    shift = scalar_ref[0]
    per_step = phase_ref.shape[1]
    parts = []
    for i in range(per_step * sub):
        bin_low = step * per_step * sub + i
        source = lax.rem(bin_low - shift + 2 * outer, outer)
        twist = (twist_ref[0, pl.ds(bin_low, 1), :], twist_ref[1, pl.ds(bin_low, 1), :])
        value = complex_mul((stage_ref[source, 0], stage_ref[source, 1]), twist)
        parts.append(jnp.concatenate(value, axis=1).astype(BF16))
    data = jnp.concatenate(parts, axis=0)
    across = ((1,), (1,))
    product = dot_f32(table_ref[0], data, across) + dot_f32(table_ref[1], data, across)
    steps = outer // sub
    pitch = order_ref.shape[0] // LANES
    far = (far_ref[0], far_ref[1])
    for i in range(per_step):
        lanes = slice(i * LANES, (i + 1) * LANES)
        at = step * per_step + i
        near = (near_ref[0, pl.ds(at, 1), :], near_ref[1, pl.ds(at, 1), :])
        turn = complex_mul(complex_mul(far, near), (phase_ref[0, i], phase_ref[1, i]))
        real, imag = complex_mul((product[:LANES, lanes], product[LANES:, lanes]), turn)
        order_ref[pl.ds(2 * at, LANES, stride=pitch), :] = real
        order_ref[pl.ds(2 * at + 1, LANES, stride=pitch), :] = imag

    @pl.when(step == pl.num_programs(0) - 1)
    def _():
        width = 2 * steps
        owned = own_ref.shape[0] // width
        for n in range(LANES):
            value = order_ref[n * pitch:n * pitch + width, :].astype(BF16)
            if n < owned:
                own_ref[n * width:(n + 1) * width, :] = value
            else:
                spill_ref[(n - owned) * width:(n - owned + 1) * width, :] = value


def range_tables():
    cos, sin = unit_roots(LANES, LANES, LANES, -1.0)
    table = np.zeros((2, LANES, 2, LANES))
    table[0, :, 0], table[0, :, 1] = cos, -sin
    table[1, :, 0], table[1, :, 1] = sin, cos
    return np.stack(split_const(table.reshape(2 * LANES, 2 * LANES)))


def range_stage(scalars, echoes, chunk, received, twist, near, far, phase, gate, sub, owned_rows):
    sources = len(received) + 1
    outer = twist.shape[1]
    steps = outer // sub
    per_step = 2
    pitch = 2 * steps + 8
    table = range_tables()
    rows = echoes.shape[3]
    whole = lambda shape: pl.BlockSpec(shape, lambda i, s: (0,) * len(shape))
    mine = pl.BlockSpec((2, None, None) + echoes.shape[3:], lambda i, s: (0, s[1], chunk, 0, 0))
    spill_rows = steps * LANES - owned_rows
    return pl.pallas_call(
        functools.partial(range_kernel, outer, sub, sources),
        grid_spec=pltpu.PrefetchScalarGridSpec(
            num_scalar_prefetch=1,
            grid=(steps // per_step,),
            in_specs=[
                mine,
                *[whole(block.shape) for block in received],
                whole(twist.shape),
                whole(near.shape),
                whole(far.shape),
                pl.BlockSpec((2, per_step, LANES, LANES), lambda i, s: (0, i, 0, 0)),
                whole(table.shape),
                pl.BlockSpec(memory_space=pl.ANY),
            ],
            out_specs=[whole((2 * owned_rows, LANES)), whole((2 * spill_rows, LANES))],
            scratch_shapes=[
                pltpu.VMEM((outer, 2, rows, LANES), F32),
                pltpu.VMEM((sources, outer // sources, 2, 16, LANES), F32),
                pltpu.VMEM((LANES * pitch, LANES), F32),
            ],
        ),
        out_shape=[jax.ShapeDtypeStruct((2 * owned_rows, LANES), BF16),
                   jax.ShapeDtypeStruct((2 * spill_rows, LANES), BF16)],
        compiler_params=pltpu.CompilerParams(
            dimension_semantics=("arbitrary",), vmem_limit_bytes=16 * 1024 * 1024),
        name="range_stage",
    )(scalars, echoes, *received, twist, near, far, phase, jnp.asarray(table), gate)


def stitch_kernel(sub, edge, scalar_ref, own_ref, low_ref, high_ref, out_ref):
    step = pl.program_id(0)
    count = pl.num_programs(0)
    shape = own_ref.shape
    lane = lax.broadcasted_iota(jnp.int32, shape, 1)
    row = lax.broadcasted_iota(jnp.int32, shape, 0)
    index = row // 2 * sub + lane // (LANES // sub)
    per_step = shape[0] // 2 * sub

    @pl.when(step < edge)
    def _():
        keep = index < scalar_ref[2] - step * per_step
        added = jnp.where(keep, low_ref[...].astype(F32), 0.0)
        out_ref[...] = (own_ref[...].astype(F32) + added).astype(BF16)

    @pl.when(jnp.logical_and(step >= edge, step < count - edge))
    def _():
        out_ref[...] = own_ref[...]

    @pl.when(step >= count - edge)
    def _():
        keep = index >= scalar_ref[3] - (step - (count - edge)) * per_step
        added = jnp.where(keep, high_ref[...].astype(F32), 0.0)
        out_ref[...] = (own_ref[...].astype(F32) + added).astype(BF16)


def stitch(scalars, own, from_below, from_above, sub):
    edge = 1
    height = from_below.shape[0] // edge
    count = own.shape[0] // height
    tile = lambda index: pl.BlockSpec((height, LANES), index)
    return pl.pallas_call(
        functools.partial(stitch_kernel, sub, edge),
        grid_spec=pltpu.PrefetchScalarGridSpec(
            num_scalar_prefetch=1,
            grid=(count,),
            in_specs=[
                tile(lambda i, s: (i, 0)),
                tile(lambda i, s: (jnp.minimum(i, edge - 1), 0)),
                tile(lambda i, s: (jnp.maximum(i - (count - edge), 0), 0)),
            ],
            out_specs=tile(lambda i, s: (i, 0)),
        ),
        out_shape=jax.ShapeDtypeStruct(own.shape, BF16),
        compiler_params=pltpu.CompilerParams(
            dimension_semantics=("arbitrary",), vmem_limit_bytes=8 * 1024 * 1024),
        name="stitch",
    )(scalars, own, from_below, from_above)


def azimuth_kernel(outer, first_ref, fore_ref, twist_ref, filter_ref, back_ref, last_ref, *refs):
    data_refs = refs[:-1]
    out_ref = refs[-1]
    chunks = len(data_refs)
    width = LANES // chunks
    count = data_refs[0].shape[0]
    twist = (twist_ref[0], twist_ref[1])
    twist_back = (twist_ref[0], -twist_ref[1])
    turn = (filter_ref[0], filter_ref[1])
    left = ((1,), (0,))
    two = lambda lhs, rhs: dot_f32(lhs[0], rhs, left) + dot_f32(lhs[1], rhs, left)
    rows = []
    for c in range(count):
        data = [ref[c] for ref in data_refs]
        spread = two((first_ref[0], first_ref[1]), jnp.concatenate(data, axis=1))
        for h in range(chunks):
            pieces = [spread[:, q * LANES + h * width:q * LANES + (h + 1) * width]
                      for q in range(chunks)]
            joined = jnp.concatenate(pieces, axis=1)
            value = complex_mul((joined[:outer], joined[outer:]), twist)
            rows.append(jnp.concatenate(value, axis=1).astype(BF16))
    total = count * chunks
    stacked = jnp.concatenate(rows, axis=0)
    doppler = dot_f32(stacked, fore_ref[0], left) + dot_f32(stacked, fore_ref[1], left)
    rows = []
    for c in range(total):
        part = doppler[c * outer:(c + 1) * outer]
        value = complex_mul((part[:, :LANES], part[:, LANES:]), turn)
        rows.append(jnp.concatenate(value, axis=1).astype(BF16))
    stacked = jnp.concatenate(rows, axis=0)
    image = dot_f32(stacked, back_ref[0], left) + dot_f32(stacked, back_ref[1], left)
    for c in range(0, total, 2):
        values = []
        for d in range(2):
            part = image[(c + d) * outer:(c + d + 1) * outer]
            value = complex_mul((part[:, :LANES], part[:, LANES:]), twist_back)
            values.append(jnp.concatenate(value, axis=0).astype(BF16))
        value = two((last_ref[0], last_ref[1]), jnp.concatenate(values, axis=1)).astype(BF16)
        out_ref[c] = value[:, :LANES]
        out_ref[c + 1] = value[:, LANES:]


def azimuth_tables(outer):
    cos, sin = unit_roots(outer, outer, outer, -1.0)
    first = np.zeros((2, outer, outer, 2))
    first[0, :, :, 0], first[0, :, :, 1] = cos, -sin
    first[1, :, :, 0], first[1, :, :, 1] = sin, cos
    last = np.zeros((outer, 2, 2, outer))
    last[:, 0, 0], last[:, 0, 1] = cos, sin
    last[:, 1, 0], last[:, 1, 1] = -sin, cos
    cos, sin = unit_roots(LANES, LANES, LANES, -1.0)
    fore = np.zeros((2, LANES, 2, LANES))
    fore[0, :, 0], fore[0, :, 1] = cos, sin
    fore[1, :, 0], fore[1, :, 1] = -sin, cos
    back = np.zeros((2, LANES, 2, LANES))
    back[0, :, 0], back[0, :, 1] = cos, -sin
    back[1, :, 0], back[1, :, 1] = sin, cos
    pair = lambda table, shape: np.stack(split_const(table.reshape(shape)))
    twist = np.stack(unit_roots(outer, LANES, outer * LANES, -1.0)).astype(np.float32)
    square = (2 * LANES, 2 * LANES)
    side = (2 * outer, 2 * outer)
    return pair(first, side), pair(fore, square), twist, pair(back, square), pair(last, side)


def azimuth_stage(data, turn, outer):
    chunks = len(data)
    count = data[0].shape[0]
    block = 8 // chunks
    first, fore, twist, back, last = azimuth_tables(outer)
    whole = lambda shape: pl.BlockSpec(shape, lambda i: (0,) * len(shape))
    tile = pl.BlockSpec((block,) + data[0].shape[1:], lambda i: (i, 0, 0))
    out_shape = (count * chunks,) + data[0].shape[1:]
    return pl.pallas_call(
        functools.partial(azimuth_kernel, outer),
        grid=(count // block,),
        in_specs=[whole(first.shape), whole(fore.shape), whole(twist.shape), whole(turn.shape),
                  whole(back.shape), whole(last.shape)] + [tile] * chunks,
        out_specs=pl.BlockSpec((block * chunks,) + out_shape[1:], lambda i: (i, 0, 0)),
        out_shape=jax.ShapeDtypeStruct(out_shape, BF16),
        compiler_params=pltpu.CompilerParams(
            dimension_semantics=("arbitrary",), vmem_limit_bytes=16 * 1024 * 1024),
        name="azimuth_stage",
    )(jnp.asarray(first), jnp.asarray(fore), jnp.asarray(twist), turn, jnp.asarray(back),
      jnp.asarray(last), *data)


def shifted(block, distance):
    devices = range(lax.axis_size("band"))
    route = [(i - distance, i) for i in devices if i - distance in devices]
    return lax.ppermute(block, "band", route)


def body(echoes, range_phase, pulse_shift, bin_offset, doppler_phase):
    range_count = lax.axis_size("range")
    group_size = lax.axis_size("pulse") * range_count
    cells_local = echoes.shape[3]
    cell_count = cells_local * range_count
    n_local = echoes.shape[2] // range_count
    spill_len = 2 * MARGIN
    owned_bins = cell_count - spill_len
    bins_local = owned_bins // group_size
    outer = cell_count // LANES
    sub = CHUNKS
    piece = n_local // sub
    steps = outer // sub
    owned_rows = owned_bins // sub

    band = lax.axis_index("band")
    bands = bin_offset.shape[0]
    order = jnp.arange(bands, dtype=jnp.int32)
    offset_of = lambda index: jnp.sum(jnp.where(order == index, bin_offset, 0))
    offset = offset_of(band)
    below = offset_of(band - 1)
    above = offset_of(band + 1)
    shift = offset - spill_len

    place = lax.axis_index("range")
    low = jnp.arange(outer, dtype=jnp.int32)
    lane = jnp.arange(LANES, dtype=jnp.int32)
    phase = jnp.concatenate((range_phase[0], range_phase[0]))
    phase = lax.dynamic_slice_in_dim(phase, spill_len - offset, cell_count, 0)
    phase = lax.optimization_barrier(jnp.transpose(phase.reshape(LANES, outer)))
    scale = 1.0 / math.sqrt(cell_count)
    phase = phase.reshape(steps, sub, LANES)
    part = lane // piece
    cube = (steps, LANES, LANES)
    spread = []
    for value in (jnp.cos(phase) * scale, jnp.sin(phase) * scale):
        wide = jnp.broadcast_to(value[:, sub - 1][..., None], cube)
        for h in range(sub - 1):
            wide = jnp.where(part == h, value[:, h][..., None], wide)
        spread.append(wide)
    spread = jnp.stack(spread)
    low_bin = jnp.arange(steps, dtype=jnp.int32)[:, None] * sub + part - shift

    def ramp(product):
        angle = jnp.mod(product, cell_count).astype(F32) * (-2.0 * math.pi / cell_count)
        return jnp.stack((jnp.cos(angle), jnp.sin(angle)))

    doppler = jnp.transpose(doppler_phase.reshape(LANES, group_size))
    factor = 1.0 / doppler_phase.shape[0]
    turn = jnp.stack((jnp.cos(doppler) * factor, jnp.sin(doppler) * factor))

    received = []
    source = echoes[0]
    for q in range(sub):
        blocks = []
        for d in range(1, range_count):
            begin = jnp.mod(place + d, range_count) * n_local + q * piece
            block = lax.dynamic_slice_in_dim(source, begin, piece, 1)
            route = [(i, (i + d) % range_count) for i in range(range_count)]
            blocks.append(lax.ppermute(block, "range", route))
        received.append(blocks[::-1])
        source = lax.optimization_barrier(source)
    held = echoes[0].reshape(2, range_count, sub, piece, cells_local)
    scalars = jnp.stack((shift, place, below, above))

    twist = ramp((low[:, None] - shift) * (lane[None, :] + cells_local * place))
    samples = []
    gate = None
    for q in range(sub):
        shifts = jnp.tile(pulse_shift[0, q * piece:(q + 1) * piece], sub)
        near = ramp(low_bin * shifts)
        far = ramp(outer * lane[:, None] * shifts)
        gate = twist if gate is None else gate
        own, spill = range_stage(scalars, held, q, received[q], twist, near, far, spread,
                                 gate, sub, owned_rows)
        from_below = shifted(spill, 1)
        from_above = shifted(spill, -1)
        gate = stitch(scalars, own, from_below, from_above, sub)
        blocks = gate.reshape(group_size, bins_local // sub, 2, LANES)
        block = lax.all_to_all(
            blocks, ("pulse", "range"), split_axis=0, concat_axis=0, tiled=True)
        samples.append(jnp.transpose(block, (1, 0, 2, 3)).reshape(
            bins_local // sub, 2 * group_size, LANES))

    image = azimuth_stage(samples, turn, group_size)
    image = jnp.transpose(image.reshape(bins_local, group_size, 2, LANES), (0, 2, 1, 3))
    return image.reshape(bins_local, 2, group_size * LANES)


def solution(mesh):
    in_specs = (
        P("band", None, "pulse", "range"),
        P("band", None),
        P("band", ("pulse", "range")),
        P(),
        P(),
    )
    out_specs = P(("band", "pulse", "range"), None, None)
    return jax.shard_map(
        body, mesh=mesh, in_specs=in_specs, out_specs=out_specs, check_vma=False)
```

```python
import functools
import math

import jax
import jax.numpy as jnp
import ml_dtypes
import numpy as np
from jax import lax
from jax.experimental import pallas as pl
from jax.experimental.pallas import tpu as pltpu
from jax.sharding import PartitionSpec as P


MARGIN = 512
LANES = 128
CHUNKS = 2
F32 = jnp.float32
BF16 = jnp.bfloat16


def split_const(table):
    high = table.astype(ml_dtypes.bfloat16)
    low = (table - high.astype(np.float64)).astype(ml_dtypes.bfloat16)
    return high, low


def unit_roots(rows, cols, modulus, sign):
    product = np.outer(np.arange(rows), np.arange(cols)) % modulus
    angle = sign * 2.0 * np.pi * product / modulus
    return np.cos(angle), np.sin(angle)


def dot_f32(lhs, rhs, contract):
    return lax.dot_general(lhs, rhs, (contract, ((), ())), preferred_element_type=F32)


def complex_mul(a, b):
    return a[0] * b[0] - a[1] * b[1], a[0] * b[1] + a[1] * b[0]


def by_constant(a, angle):
    cos = math.cos(angle)
    sin = math.sin(angle)
    quarter = angle / (math.pi / 2)
    if abs(quarter - round(quarter)) < 1e-9:
        turn = int(round(quarter)) % 4
        if turn == 0:
            return a
        if turn == 1:
            return -a[1], a[0]
        if turn == 2:
            return -a[0], -a[1]
        return a[1], -a[0]
    if abs(abs(cos) - abs(sin)) < 1e-9:
        half = math.sqrt(0.5)
        plus = (a[0] + a[1]) * half
        minus = (a[0] - a[1]) * half
        if cos > 0 and sin > 0:
            return minus, plus
        if cos < 0 and sin > 0:
            return -plus, minus
        if cos < 0 and sin < 0:
            return -minus, -plus
        return plus, -minus
    return a[0] * cos - a[1] * sin, a[0] * sin + a[1] * cos


def small_dft(values, sign):
    count = len(values)
    if count == 1:
        return values
    even = small_dft(values[0::2], sign)
    odd = small_dft(values[1::2], sign)
    first = []
    second = []
    for i in range(count // 2):
        turned = by_constant(odd[i], sign * 2.0 * math.pi * i / count)
        first.append((even[i][0] + turned[0], even[i][1] + turned[1]))
        second.append((even[i][0] - turned[0], even[i][1] - turned[1]))
    return first + second


def turned_rows(product, lanes, rows, at, near_ref, far_ref, phase_ref):
    span = rows.stop - rows.start
    total = product[:2 * span, lanes] + product[2 * span:, lanes]
    near = (near_ref[0, at:at + 1, :], near_ref[1, at:at + 1, :])
    far = (far_ref[0, rows, :], far_ref[1, rows, :])
    phase = (phase_ref[0, at, rows, :], phase_ref[1, at, rows, :])
    return complex_mul((total[:span], total[span:]), complex_mul(complex_mul(far, near), phase))


def ordered_rows(out_ref, order_ref, width):
    pitch = width + 8
    for n in range(out_ref.shape[0] // width):
        out_ref[n * width:(n + 1) * width, :] = (
            order_ref[n * pitch:n * pitch + width, :].astype(BF16))


def cells_kernel(outer, sub, sources, first, scalar_ref, mine_ref, *refs):
    echo_refs = (mine_ref,) + refs[:sources - 1]
    (twist_ref, near_ref, far_ref, phase_ref, table_ref, _, data_ref, spill_ref,
     stage_ref, mid_ref, order_ref) = refs[sources - 1:]
    rows = echo_refs[0].shape[1]
    inner = outer // sources
    group = 16

    def block(t, carry):
        at = pl.multiple_of(t * group, group)
        for n in range(inner):
            lanes = slice(n * LANES, (n + 1) * LANES)
            values = []
            for echo_ref in echo_refs:
                values.append((
                    echo_ref[0, pl.ds(at, group), lanes].astype(F32),
                    echo_ref[1, pl.ds(at, group), lanes].astype(F32),
                ))
            for q, value in enumerate(small_dft(values, -1.0)):
                value = by_constant(value, -2.0 * math.pi * n * q / outer)
                mid_ref[q, n, 0] = value[0]
                mid_ref[q, n, 1] = value[1]
        for q in range(sources):
            values = [(mid_ref[q, n, 0], mid_ref[q, n, 1]) for n in range(inner)]
            for m, value in enumerate(small_dft(values, -1.0)):
                stage_ref[q + sources * m, 0, pl.ds(at, group), :] = value[0]
                stage_ref[q + sources * m, 1, pl.ds(at, group), :] = value[1]
        return carry

    lax.fori_loop(0, rows // group, block, 0)
    shift = scalar_ref[0]
    steps = outer // sub
    pitch = 2 * steps + 8
    kept = slice(first, LANES)
    count = LANES - first
    for step in range(0, steps, 2):
        parts = []
        for i in range(2):
            halves = []
            for h in range(sub):
                bin_low = (step + i) * sub + h
                source = lax.rem(bin_low - shift + 2 * outer, outer)
                twist = (twist_ref[0, bin_low:bin_low + 1, :], twist_ref[1, bin_low:bin_low + 1, :])
                value = complex_mul((stage_ref[source, 0], stage_ref[source, 1]), twist)
                halves.append(jnp.concatenate(value, axis=1).astype(BF16))
            part = jnp.concatenate(halves, axis=0)
            data_ref[step + i] = part
            parts.append(part)
        product = dot_f32(table_ref[...], jnp.concatenate(parts, axis=0), ((1,), (1,)))
        for i in range(2):
            at = step + i
            lanes = slice(i * LANES, (i + 1) * LANES)
            value = turned_rows(product, lanes, kept, at, near_ref, far_ref, phase_ref)
            order_ref[pl.ds(2 * at, count, stride=pitch), :] = value[0]
            order_ref[pl.ds(2 * at + 1, count, stride=pitch), :] = value[1]
    ordered_rows(spill_ref, order_ref, 2 * steps)


def owned_kernel(data_ref, near_ref, far_ref, phase_ref, table_ref, out_ref, order_ref):
    steps = data_ref.shape[0]
    pitch = 2 * steps + 8
    count = table_ref.shape[0] // 4
    kept = slice(0, count)
    for step in range(0, steps, 2):
        data = jnp.concatenate((data_ref[step], data_ref[step + 1]), axis=0)
        product = dot_f32(table_ref[...], data, ((1,), (1,)))
        for i in range(2):
            at = step + i
            lanes = slice(i * LANES, (i + 1) * LANES)
            value = turned_rows(product, lanes, kept, at, near_ref, far_ref, phase_ref)
            order_ref[pl.ds(2 * at, count, stride=pitch), :] = value[0]
            order_ref[pl.ds(2 * at + 1, count, stride=pitch), :] = value[1]
    ordered_rows(out_ref, order_ref, 2 * steps)


def range_tables(first):
    cos, sin = unit_roots(LANES, LANES, LANES, -1.0)
    table = np.zeros((2, LANES, 2, LANES))
    table[0, :, 0], table[0, :, 1] = cos, -sin
    table[1, :, 0], table[1, :, 1] = sin, cos
    stack = lambda part: np.concatenate(split_const(part.reshape(-1, 2 * LANES)))
    return stack(table[:, :first]), stack(table[:, first:])


def cells_stage(scalars, echoes, chunk, received, twist, near, far, phase, gate, sub, first):
    sources = len(received) + 1
    outer = twist.shape[1]
    steps = outer // sub
    table = jnp.asarray(range_tables(first)[1])
    rows = echoes.shape[3]
    whole = lambda shape: pl.BlockSpec(shape, lambda i, s: (0,) * len(shape))
    mine = pl.BlockSpec((2, None, None) + echoes.shape[3:], lambda i, s: (0, s[1], chunk, 0, 0))
    operands = (*received, twist, near, far, phase, table)
    data = jax.ShapeDtypeStruct((steps, LANES, 2 * LANES), BF16)
    spill = jax.ShapeDtypeStruct((2 * steps * (LANES - first), LANES), BF16)
    return pl.pallas_call(
        functools.partial(cells_kernel, outer, sub, sources, first),
        grid_spec=pltpu.PrefetchScalarGridSpec(
            num_scalar_prefetch=1,
            grid=(1,),
            in_specs=[mine, *[whole(value.shape) for value in operands],
                      pl.BlockSpec(memory_space=pl.ANY)],
            out_specs=[whole(data.shape), whole(spill.shape)],
            scratch_shapes=[
                pltpu.VMEM((outer, 2, rows, LANES), F32),
                pltpu.VMEM((sources, outer // sources, 2, 16, LANES), F32),
                pltpu.VMEM(((LANES - first) * (2 * steps + 8), LANES), F32),
            ],
        ),
        out_shape=[data, spill],
        compiler_params=pltpu.CompilerParams(
            dimension_semantics=("arbitrary",), vmem_limit_bytes=16 * 1024 * 1024),
        name="cells_stage",
    )(scalars, echoes, *operands, gate)


def owned_stage(data, near, far, phase, first):
    steps = data.shape[0]
    table = jnp.asarray(range_tables(first)[0])
    vmem = pl.BlockSpec(memory_space=pltpu.VMEM)
    return pl.pallas_call(
        owned_kernel,
        in_specs=[vmem] * 5,
        out_specs=vmem,
        out_shape=jax.ShapeDtypeStruct((2 * steps * first, LANES), BF16),
        scratch_shapes=[pltpu.VMEM((first * (2 * steps + 8), LANES), F32)],
        compiler_params=pltpu.CompilerParams(vmem_limit_bytes=12 * 1024 * 1024),
        name="owned_stage",
    )(data, near, far, phase, table)


def stitch_kernel(sub, scalar_ref, own_ref, low_ref, high_ref, out_ref, first_ref, last_ref, sems):
    height = low_ref.shape[0]
    last = own_ref.shape[0] - height
    lane = lax.broadcasted_iota(jnp.int32, low_ref.shape, 1)
    row = lax.broadcasted_iota(jnp.int32, low_ref.shape, 0)
    index = row // 2 * sub + lane // (LANES // sub)
    middle = pltpu.make_async_copy(
        own_ref.at[height:last], out_ref.at[height:last], sems.at[0])
    middle.start()
    added = jnp.where(index < scalar_ref[2], low_ref[...].astype(F32), 0.0)
    first_ref[...] = (own_ref[:height].astype(F32) + added).astype(BF16)
    begin = pltpu.make_async_copy(first_ref, out_ref.at[:height], sems.at[1])
    begin.start()
    added = jnp.where(index >= scalar_ref[3], high_ref[...].astype(F32), 0.0)
    last_ref[...] = (own_ref[last:].astype(F32) + added).astype(BF16)
    end = pltpu.make_async_copy(last_ref, out_ref.at[last:], sems.at[2])
    end.start()
    middle.wait()
    begin.wait()
    end.wait()


def stitch(scalars, own, from_below, from_above, sub):
    vmem = pl.BlockSpec(memory_space=pltpu.VMEM)
    return pl.pallas_call(
        functools.partial(stitch_kernel, sub),
        in_specs=[pl.BlockSpec(memory_space=pltpu.SMEM), vmem, vmem, vmem],
        out_specs=pl.BlockSpec(memory_space=pl.ANY),
        out_shape=jax.ShapeDtypeStruct(own.shape, BF16),
        scratch_shapes=[pltpu.VMEM(from_below.shape, BF16), pltpu.VMEM(from_below.shape, BF16),
                        pltpu.SemaphoreType.DMA((3,))],
        compiler_params=pltpu.CompilerParams(vmem_limit_bytes=8 * 1024 * 1024),
        name="stitch",
    )(scalars, own, from_below, from_above)


def azimuth_kernel(outer, first_ref, fore_ref, twist_ref, filter_ref, back_ref, last_ref, *refs):
    data_refs = refs[:-1]
    out_ref = refs[-1]
    chunks = len(data_refs)
    width = LANES // chunks
    count = data_refs[0].shape[0]
    twist = (twist_ref[0], twist_ref[1])
    twist_back = (twist_ref[0], -twist_ref[1])
    turn = (filter_ref[0], filter_ref[1])
    left = ((1,), (0,))
    two = lambda lhs, rhs: dot_f32(lhs[0], rhs, left) + dot_f32(lhs[1], rhs, left)
    rows = []
    for c in range(count):
        data = [ref[c] for ref in data_refs]
        spread = two((first_ref[0], first_ref[1]), jnp.concatenate(data, axis=1))
        for h in range(chunks):
            pieces = [spread[:, q * LANES + h * width:q * LANES + (h + 1) * width]
                      for q in range(chunks)]
            joined = jnp.concatenate(pieces, axis=1)
            value = complex_mul((joined[:outer], joined[outer:]), twist)
            rows.append(jnp.concatenate(value, axis=1).astype(BF16))
    total = count * chunks
    stacked = jnp.concatenate(rows, axis=0)
    doppler = dot_f32(stacked, fore_ref[0], left) + dot_f32(stacked, fore_ref[1], left)
    rows = []
    for c in range(total):
        part = doppler[c * outer:(c + 1) * outer]
        value = complex_mul((part[:, :LANES], part[:, LANES:]), turn)
        rows.append(jnp.concatenate(value, axis=1).astype(BF16))
    stacked = jnp.concatenate(rows, axis=0)
    image = dot_f32(stacked, back_ref[0], left) + dot_f32(stacked, back_ref[1], left)
    for c in range(0, total, 2):
        values = []
        for d in range(2):
            part = image[(c + d) * outer:(c + d + 1) * outer]
            value = complex_mul((part[:, :LANES], part[:, LANES:]), twist_back)
            values.append(jnp.concatenate(value, axis=0).astype(BF16))
        value = two((last_ref[0], last_ref[1]), jnp.concatenate(values, axis=1)).astype(BF16)
        out_ref[c] = value[:, :LANES]
        out_ref[c + 1] = value[:, LANES:]


def azimuth_tables(outer):
    cos, sin = unit_roots(outer, outer, outer, -1.0)
    first = np.zeros((2, outer, outer, 2))
    first[0, :, :, 0], first[0, :, :, 1] = cos, -sin
    first[1, :, :, 0], first[1, :, :, 1] = sin, cos
    last = np.zeros((outer, 2, 2, outer))
    last[:, 0, 0], last[:, 0, 1] = cos, sin
    last[:, 1, 0], last[:, 1, 1] = -sin, cos
    cos, sin = unit_roots(LANES, LANES, LANES, -1.0)
    fore = np.zeros((2, LANES, 2, LANES))
    fore[0, :, 0], fore[0, :, 1] = cos, sin
    fore[1, :, 0], fore[1, :, 1] = -sin, cos
    back = np.zeros((2, LANES, 2, LANES))
    back[0, :, 0], back[0, :, 1] = cos, -sin
    back[1, :, 0], back[1, :, 1] = sin, cos
    pair = lambda table, shape: np.stack(split_const(table.reshape(shape)))
    twist = np.stack(unit_roots(outer, LANES, outer * LANES, -1.0)).astype(np.float32)
    square = (2 * LANES, 2 * LANES)
    side = (2 * outer, 2 * outer)
    return pair(first, side), pair(fore, square), twist, pair(back, square), pair(last, side)


def azimuth_stage(data, turn, outer):
    chunks = len(data)
    count = data[0].shape[0]
    block = 16 // chunks
    first, fore, twist, back, last = azimuth_tables(outer)
    whole = lambda shape: pl.BlockSpec(shape, lambda i: (0,) * len(shape))
    tile = pl.BlockSpec((block,) + data[0].shape[1:], lambda i: (i, 0, 0))
    out_shape = (count * chunks,) + data[0].shape[1:]
    return pl.pallas_call(
        functools.partial(azimuth_kernel, outer),
        grid=(count // block,),
        in_specs=[whole(first.shape), whole(fore.shape), whole(twist.shape), whole(turn.shape),
                  whole(back.shape), whole(last.shape)] + [tile] * chunks,
        out_specs=pl.BlockSpec((block * chunks,) + out_shape[1:], lambda i: (i, 0, 0)),
        out_shape=jax.ShapeDtypeStruct(out_shape, BF16),
        compiler_params=pltpu.CompilerParams(
            dimension_semantics=("arbitrary",), vmem_limit_bytes=16 * 1024 * 1024),
        name="azimuth_stage",
    )(jnp.asarray(first), jnp.asarray(fore), jnp.asarray(twist), turn, jnp.asarray(back),
      jnp.asarray(last), *data)


def shifted(block, distance):
    devices = range(lax.axis_size("band"))
    route = [(i - distance, i) for i in devices if i - distance in devices]
    return lax.ppermute(block, "band", route)


def body(echoes, range_phase, pulse_shift, bin_offset, doppler_phase):
    range_count = lax.axis_size("range")
    group_size = lax.axis_size("pulse") * range_count
    cells_local = echoes.shape[3]
    cell_count = cells_local * range_count
    n_local = echoes.shape[2] // range_count
    spill_len = 2 * MARGIN
    owned_bins = cell_count - spill_len
    bins_local = owned_bins // group_size
    outer = cell_count // LANES
    sub = CHUNKS
    piece = n_local // sub
    steps = outer // sub

    band = lax.axis_index("band")
    bands = bin_offset.shape[0]
    order = jnp.arange(bands, dtype=jnp.int32)
    offset_of = lambda index: jnp.sum(jnp.where(order == index, bin_offset, 0))
    offset = offset_of(band)
    below = offset_of(band - 1)
    above = offset_of(band + 1)
    shift = offset - spill_len

    place = lax.axis_index("range")
    low = jnp.arange(outer, dtype=jnp.int32)
    lane = jnp.arange(LANES, dtype=jnp.int32)
    phase = jnp.concatenate((range_phase[0], range_phase[0]))
    phase = lax.dynamic_slice_in_dim(phase, spill_len - offset, cell_count, 0)
    phase = lax.optimization_barrier(jnp.transpose(phase.reshape(LANES, outer)))
    scale = 1.0 / math.sqrt(cell_count)
    phase = phase.reshape(steps, sub, LANES)
    part = lane // piece
    cube = (steps, LANES, LANES)
    spread = []
    for value in (jnp.cos(phase) * scale, jnp.sin(phase) * scale):
        wide = jnp.broadcast_to(value[:, sub - 1][..., None], cube)
        for h in range(sub - 1):
            wide = jnp.where(part == h, value[:, h][..., None], wide)
        spread.append(wide)
    spread = jnp.stack(spread)
    low_bin = jnp.arange(steps, dtype=jnp.int32)[:, None] * sub + part - shift

    def ramp(product):
        angle = jnp.mod(product, cell_count).astype(F32) * (-2.0 * math.pi / cell_count)
        return jnp.stack((jnp.cos(angle), jnp.sin(angle)))

    doppler = jnp.transpose(doppler_phase.reshape(LANES, group_size))
    factor = 1.0 / doppler_phase.shape[0]
    turn = jnp.stack((jnp.cos(doppler) * factor, jnp.sin(doppler) * factor))

    received = []
    source = echoes[0]
    for q in range(sub):
        blocks = []
        for d in range(range_count - 1, 0, -1):
            begin = jnp.mod(place + d, range_count) * n_local + q * piece
            block = lax.dynamic_slice_in_dim(source, begin, piece, 1)
            route = [(i, (i + d) % range_count) for i in range(range_count)]
            blocks.append(lax.ppermute(block, "range", route))
            if d == 1:
                source = lax.optimization_barrier(source)
        received.append(blocks)
    held = echoes[0].reshape(2, range_count, sub, piece, cells_local)
    scalars = jnp.stack((shift, place, below, above))

    twist = ramp((low[:, None] - shift) * (lane[None, :] + cells_local * place))
    samples = []
    gate = None
    for q in range(sub):
        shifts = jnp.tile(pulse_shift[0, q * piece:(q + 1) * piece], sub)
        near = ramp(low_bin * shifts)
        far = ramp(outer * lane[:, None] * shifts)
        gate = twist if gate is None else gate
        first = owned_bins // outer
        data, spill = cells_stage(scalars, held, q, received[q], twist, near, far, spread,
                                  gate, sub, first)
        own = owned_stage(data, near, far, spread, first)
        from_below = shifted(spill, 1)
        from_above = shifted(spill, -1)
        gate = stitch(scalars, own, from_below, from_above, sub)
        blocks = gate.reshape(group_size, bins_local // sub, 2, LANES)
        block = lax.all_to_all(
            blocks, ("pulse", "range"), split_axis=0, concat_axis=0, tiled=True)
        samples.append(jnp.transpose(block, (1, 0, 2, 3)).reshape(
            bins_local // sub, 2 * group_size, LANES))

    image = azimuth_stage(samples, turn, group_size)
    image = jnp.transpose(image.reshape(bins_local, group_size, 2, LANES), (0, 2, 1, 3))
    return image.reshape(bins_local, 2, group_size * LANES)


def solution(mesh):
    in_specs = (
        P("band", None, "pulse", "range"),
        P("band", None),
        P("band", ("pulse", "range")),
        P(),
        P(),
    )
    out_specs = P(("band", "pulse", "range"), None, None)
    return jax.shard_map(
        body, mesh=mesh, in_specs=in_specs, out_specs=out_specs, check_vma=False)
```

```python
import functools
import math

import jax
import jax.numpy as jnp
import ml_dtypes
import numpy as np
from jax import lax
from jax.experimental import pallas as pl
from jax.experimental.pallas import tpu as pltpu
from jax.sharding import PartitionSpec as P


MARGIN = 512
LANES = 128
CHUNKS = 2
F32 = jnp.float32
BF16 = jnp.bfloat16


def split_const(table):
    high = table.astype(ml_dtypes.bfloat16)
    low = (table - high.astype(np.float64)).astype(ml_dtypes.bfloat16)
    return high, low


def unit_roots(rows, cols, modulus, sign):
    product = np.outer(np.arange(rows), np.arange(cols)) % modulus
    angle = sign * 2.0 * np.pi * product / modulus
    return np.cos(angle), np.sin(angle)


def dot_f32(lhs, rhs, contract):
    return lax.dot_general(lhs, rhs, (contract, ((), ())), preferred_element_type=F32)


def complex_mul(a, b):
    return a[0] * b[0] - a[1] * b[1], a[0] * b[1] + a[1] * b[0]


def by_constant(a, angle):
    cos = math.cos(angle)
    sin = math.sin(angle)
    quarter = angle / (math.pi / 2)
    if abs(quarter - round(quarter)) < 1e-9:
        turn = int(round(quarter)) % 4
        if turn == 0:
            return a
        if turn == 1:
            return -a[1], a[0]
        if turn == 2:
            return -a[0], -a[1]
        return a[1], -a[0]
    if abs(abs(cos) - abs(sin)) < 1e-9:
        half = math.sqrt(0.5)
        plus = (a[0] + a[1]) * half
        minus = (a[0] - a[1]) * half
        if cos > 0 and sin > 0:
            return minus, plus
        if cos < 0 and sin > 0:
            return -plus, minus
        if cos < 0 and sin < 0:
            return -minus, -plus
        return plus, -minus
    return a[0] * cos - a[1] * sin, a[0] * sin + a[1] * cos


def small_dft(values, sign):
    count = len(values)
    if count == 1:
        return values
    even = small_dft(values[0::2], sign)
    odd = small_dft(values[1::2], sign)
    first = []
    second = []
    for i in range(count // 2):
        turned = by_constant(odd[i], sign * 2.0 * math.pi * i / count)
        first.append((even[i][0] + turned[0], even[i][1] + turned[1]))
        second.append((even[i][0] - turned[0], even[i][1] - turned[1]))
    return first + second


def turned_rows(product, lanes, rows, at, near_ref, far_ref, phase_ref):
    span = rows.stop - rows.start
    total = product[:2 * span, lanes] + product[2 * span:, lanes]
    near = (near_ref[0, at:at + 1, :], near_ref[1, at:at + 1, :])
    far = (far_ref[0, rows, :], far_ref[1, rows, :])
    phase = (phase_ref[0, at, rows, :], phase_ref[1, at, rows, :])
    return complex_mul((total[:span], total[span:]), complex_mul(complex_mul(far, near), phase))


def ordered_rows(out_ref, order_ref, width):
    pitch = width + 8
    for n in range(out_ref.shape[0] // width):
        out_ref[n * width:(n + 1) * width, :] = (
            order_ref[n * pitch:n * pitch + width, :].astype(BF16))


def cells_kernel(outer, sub, sources, first, scalar_ref, mine_ref, *refs):
    echo_refs = (mine_ref,) + refs[:sources - 1]
    (twist_ref, near_ref, far_ref, phase_ref, table_ref, _, data_ref, spill_ref,
     stage_ref, mid_ref, order_ref) = refs[sources - 1:]
    rows = echo_refs[0].shape[1]
    inner = outer // sources
    group = 16

    def block(t, carry):
        at = pl.multiple_of(t * group, group)
        for n in range(inner):
            lanes = slice(n * LANES, (n + 1) * LANES)
            values = []
            for echo_ref in echo_refs:
                values.append((
                    echo_ref[0, pl.ds(at, group), lanes].astype(F32),
                    echo_ref[1, pl.ds(at, group), lanes].astype(F32),
                ))
            for q, value in enumerate(small_dft(values, -1.0)):
                value = by_constant(value, -2.0 * math.pi * n * q / outer)
                mid_ref[q, n, 0] = value[0]
                mid_ref[q, n, 1] = value[1]
        for q in range(sources):
            values = [(mid_ref[q, n, 0], mid_ref[q, n, 1]) for n in range(inner)]
            for m, value in enumerate(small_dft(values, -1.0)):
                stage_ref[q + sources * m, 0, pl.ds(at, group), :] = value[0]
                stage_ref[q + sources * m, 1, pl.ds(at, group), :] = value[1]
        return carry

    lax.fori_loop(0, rows // group, block, 0)
    shift = scalar_ref[0]
    steps = outer // sub
    pitch = 2 * steps + 8
    kept = slice(first, LANES)
    count = LANES - first
    for step in range(0, steps, 2):
        parts = []
        for i in range(2):
            halves = []
            for h in range(sub):
                bin_low = (step + i) * sub + h
                source = lax.rem(bin_low - shift + 2 * outer, outer)
                twist = (twist_ref[0, bin_low:bin_low + 1, :], twist_ref[1, bin_low:bin_low + 1, :])
                value = complex_mul((stage_ref[source, 0], stage_ref[source, 1]), twist)
                halves.append(jnp.concatenate(value, axis=1).astype(BF16))
            part = jnp.concatenate(halves, axis=0)
            data_ref[step + i] = part
            parts.append(part)
        product = dot_f32(table_ref[...], jnp.concatenate(parts, axis=0), ((1,), (1,)))
        for i in range(2):
            at = step + i
            lanes = slice(i * LANES, (i + 1) * LANES)
            value = turned_rows(product, lanes, kept, at, near_ref, far_ref, phase_ref)
            order_ref[pl.ds(2 * at, count, stride=pitch), :] = value[0]
            order_ref[pl.ds(2 * at + 1, count, stride=pitch), :] = value[1]
    ordered_rows(spill_ref, order_ref, 2 * steps)


def owned_kernel(data_ref, near_ref, far_ref, phase_ref, table_ref, out_ref, order_ref):
    steps = data_ref.shape[0]
    pitch = 2 * steps + 8
    count = table_ref.shape[0] // 4
    kept = slice(0, count)
    for step in range(0, steps, 2):
        data = jnp.concatenate((data_ref[step], data_ref[step + 1]), axis=0)
        product = dot_f32(table_ref[...], data, ((1,), (1,)))
        for i in range(2):
            at = step + i
            lanes = slice(i * LANES, (i + 1) * LANES)
            value = turned_rows(product, lanes, kept, at, near_ref, far_ref, phase_ref)
            order_ref[pl.ds(2 * at, count, stride=pitch), :] = value[0]
            order_ref[pl.ds(2 * at + 1, count, stride=pitch), :] = value[1]
    ordered_rows(out_ref, order_ref, 2 * steps)


def range_tables(first):
    cos, sin = unit_roots(LANES, LANES, LANES, -1.0)
    table = np.zeros((2, LANES, 2, LANES))
    table[0, :, 0], table[0, :, 1] = cos, -sin
    table[1, :, 0], table[1, :, 1] = sin, cos
    stack = lambda part: np.concatenate(split_const(part.reshape(-1, 2 * LANES)))
    return stack(table[:, :first]), stack(table[:, first:])


def cells_stage(scalars, echoes, chunk, received, twist, near, far, phase, gate, sub, first):
    sources = len(received) + 1
    outer = twist.shape[1]
    steps = outer // sub
    table = jnp.asarray(range_tables(first)[1])
    rows = echoes.shape[3]
    whole = lambda shape: pl.BlockSpec(shape, lambda i, s: (0,) * len(shape))
    mine = pl.BlockSpec((2, None, None) + echoes.shape[3:], lambda i, s: (0, s[1], chunk, 0, 0))
    operands = (*received, twist, near, far, phase, table)
    data = jax.ShapeDtypeStruct((steps, LANES, 2 * LANES), BF16)
    spill = jax.ShapeDtypeStruct((2 * steps * (LANES - first), LANES), BF16)
    return pl.pallas_call(
        functools.partial(cells_kernel, outer, sub, sources, first),
        grid_spec=pltpu.PrefetchScalarGridSpec(
            num_scalar_prefetch=1,
            grid=(1,),
            in_specs=[mine, *[whole(value.shape) for value in operands],
                      pl.BlockSpec(memory_space=pl.ANY)],
            out_specs=[whole(data.shape), whole(spill.shape)],
            scratch_shapes=[
                pltpu.VMEM((outer, 2, rows, LANES), F32),
                pltpu.VMEM((sources, outer // sources, 2, 16, LANES), F32),
                pltpu.VMEM(((LANES - first) * (2 * steps + 8), LANES), F32),
            ],
        ),
        out_shape=[data, spill],
        compiler_params=pltpu.CompilerParams(
            dimension_semantics=("arbitrary",), vmem_limit_bytes=16 * 1024 * 1024),
        name="cells_stage",
    )(scalars, echoes, *operands, gate)


def owned_stage(data, near, far, phase, first):
    steps = data.shape[0]
    table = jnp.asarray(range_tables(first)[0])
    vmem = pl.BlockSpec(memory_space=pltpu.VMEM)
    return pl.pallas_call(
        owned_kernel,
        in_specs=[vmem] * 5,
        out_specs=vmem,
        out_shape=jax.ShapeDtypeStruct((2 * steps * first, LANES), BF16),
        scratch_shapes=[pltpu.VMEM((first * (2 * steps + 8), LANES), F32)],
        compiler_params=pltpu.CompilerParams(vmem_limit_bytes=12 * 1024 * 1024),
        name="owned_stage",
    )(data, near, far, phase, table)


def stitch_kernel(sub, scalar_ref, own_ref, low_ref, high_ref, out_ref, held_ref, sems):
    _, ranges, height, _ = held_ref.shape
    unit = 16
    edge = low_ref.shape[0] // unit
    count = own_ref.shape[0] // unit
    per_block = height // unit
    lane = lax.broadcasted_iota(jnp.int32, (unit, LANES), 1)
    row = lax.broadcasted_iota(jnp.int32, (unit, LANES), 0)
    index = row // 2 * sub + lane // (LANES // sub)
    per_unit = unit // 2 * sub
    for i in range(count):
        rows = slice(i * unit, (i + 1) * unit)
        value = own_ref[rows]
        if i < edge:
            added = jnp.where(index < scalar_ref[2] - i * per_unit, low_ref[rows].astype(F32), 0.0)
            value = (value.astype(F32) + added).astype(BF16)
        elif i >= count - edge:
            j = i - (count - edge)
            other = high_ref[j * unit:(j + 1) * unit].astype(F32)
            added = jnp.where(index >= scalar_ref[3] - j * per_unit, other, 0.0)
            value = (value.astype(F32) + added).astype(BF16)
        block = i // per_block
        at = i % per_block * unit
        held_ref[block // ranges, block % ranges, at:at + unit] = value
    copies = [pltpu.make_async_copy(held_ref.at[:, r], out_ref.at[r], sems.at[r])
              for r in range(ranges)]
    for copy in copies:
        copy.start()
    for copy in copies:
        copy.wait()


def stitch(scalars, own, from_below, from_above, sub, pulses, ranges):
    vmem = pl.BlockSpec(memory_space=pltpu.VMEM)
    height = own.shape[0] // (pulses * ranges)
    return pl.pallas_call(
        functools.partial(stitch_kernel, sub),
        in_specs=[pl.BlockSpec(memory_space=pltpu.SMEM), vmem, vmem, vmem],
        out_specs=pl.BlockSpec(memory_space=pl.ANY),
        out_shape=jax.ShapeDtypeStruct((ranges, pulses, height, LANES), BF16),
        scratch_shapes=[pltpu.VMEM((pulses, ranges, height, LANES), BF16),
                        pltpu.SemaphoreType.DMA((ranges,))],
        compiler_params=pltpu.CompilerParams(vmem_limit_bytes=8 * 1024 * 1024),
        name="stitch",
    )(scalars, own, from_below, from_above)


def spread_rows(first_ref, data, twist_ref):
    left = ((1,), (0,))
    wide = jnp.concatenate(data, axis=1)
    spread = dot_f32(first_ref[0], wide, left) + dot_f32(first_ref[1], wide, left)
    half = spread.shape[0] // 2
    twist = (twist_ref[0], twist_ref[1])
    rows = []
    for i in range(len(data)):
        lanes = slice(i * LANES, (i + 1) * LANES)
        real, imag = complex_mul((spread[:half, lanes], spread[half:, lanes]), twist)
        width = LANES // CHUNKS
        for h in range(CHUNKS):
            part = slice(h * width, (h + 1) * width)
            rows.append(jnp.concatenate((real[:, part], imag[:, part]), axis=1).astype(BF16))
    return rows


def spread_kernel(first_ref, twist_ref, data_ref, out_ref):
    for c in range(0, data_ref.shape[0], 2):
        rows = spread_rows(first_ref, (data_ref[c], data_ref[c + 1]), twist_ref)
        for i, value in enumerate(rows):
            out_ref[c * CHUNKS + i] = value


def azimuth_kernel(outer, first_ref, fore_ref, twist_ref, back_twist_ref, filter_ref, back_ref,
                   last_ref, *refs):
    early_refs = refs[:-2]
    data_ref, out_ref = refs[-2:]
    twist_back = (back_twist_ref[0], -back_twist_ref[1])
    turn = (filter_ref[0], filter_ref[1])
    left = ((1,), (0,))
    two = lambda lhs, rhs: dot_f32(lhs[0], rhs, left) + dot_f32(lhs[1], rhs, left)
    rows = []
    for c in range(0, data_ref.shape[0], 2):
        rows += spread_rows(first_ref, (data_ref[c], data_ref[c + 1]), twist_ref)
    total = len(rows)
    rows = [jnp.concatenate([ref[c] for ref in early_refs] + [rows[c]], axis=1)
            for c in range(total)]
    stacked = jnp.concatenate(rows, axis=0)
    doppler = dot_f32(stacked, fore_ref[0], left) + dot_f32(stacked, fore_ref[1], left)
    rows = []
    for c in range(total):
        part = doppler[c * outer:(c + 1) * outer]
        value = complex_mul((part[:, :LANES], part[:, LANES:]), turn)
        rows.append(jnp.concatenate(value, axis=1).astype(BF16))
    stacked = jnp.concatenate(rows, axis=0)
    image = dot_f32(stacked, back_ref[0], left) + dot_f32(stacked, back_ref[1], left)
    for c in range(0, total, 2):
        values = []
        for d in range(2):
            part = image[(c + d) * outer:(c + d + 1) * outer]
            value = complex_mul((part[:, :LANES], part[:, LANES:]), twist_back)
            values.append(jnp.concatenate(value, axis=0).astype(BF16))
        value = two((last_ref[0], last_ref[1]), jnp.concatenate(values, axis=1)).astype(BF16)
        out_ref[c] = value[:, :LANES]
        out_ref[c + 1] = value[:, LANES:]


def azimuth_tables(outer, ranges):
    cos, sin = unit_roots(outer, outer, outer, -1.0)
    first = np.zeros((2, outer, outer, 2))
    first[0, :, :, 0], first[0, :, :, 1] = cos, -sin
    first[1, :, :, 0], first[1, :, :, 1] = sin, cos
    slots = np.arange(outer)
    first = first[:, :, slots % (outer // ranges) * ranges + slots // (outer // ranges)]
    last = np.zeros((outer, 2, 2, outer))
    last[:, 0, 0], last[:, 0, 1] = cos, sin
    last[:, 1, 0], last[:, 1, 1] = -sin, cos
    cos, sin = unit_roots(LANES, LANES, LANES, -1.0)
    fore = np.zeros((2, LANES, 2, LANES))
    fore[0, :, 0], fore[0, :, 1] = cos, sin
    fore[1, :, 0], fore[1, :, 1] = -sin, cos
    back = np.zeros((2, LANES, 2, LANES))
    back[0, :, 0], back[0, :, 1] = cos, -sin
    back[1, :, 0], back[1, :, 1] = sin, cos
    pair = lambda table, shape: np.stack(split_const(table.reshape(shape)))
    fore = fore.reshape(2, CHUNKS, LANES // CHUNKS, 2 * LANES).transpose(1, 0, 2, 3)
    twist = np.stack(unit_roots(outer, LANES, outer * LANES, -1.0)).astype(np.float32)
    square = (2 * LANES, 2 * LANES)
    side = (2 * outer, 2 * outer)
    return pair(first, side), pair(fore, square), twist, pair(back, square), pair(last, side)


def chunk_twist(twist, chunk):
    width = LANES // CHUNKS
    return jnp.asarray(np.tile(twist[:, :, chunk * width:(chunk + 1) * width], CHUNKS))


def spread_stage(data, chunk, outer, ranges):
    first, _, twist, _, _ = azimuth_tables(outer, ranges)
    vmem = pl.BlockSpec(memory_space=pltpu.VMEM)
    return pl.pallas_call(
        spread_kernel,
        in_specs=[vmem] * 3,
        out_specs=vmem,
        out_shape=jax.ShapeDtypeStruct((data.shape[0] * CHUNKS, outer, LANES), BF16),
        compiler_params=pltpu.CompilerParams(vmem_limit_bytes=12 * 1024 * 1024),
        name="spread_stage",
    )(jnp.asarray(first), chunk_twist(twist, chunk), data)


def azimuth_stage(early, data, turn, outer, ranges):
    chunks = CHUNKS
    count = data.shape[0]
    block = 16 // chunks
    first, fore, twist, back, last = azimuth_tables(outer, ranges)
    constants = [jnp.asarray(first), jnp.asarray(fore), chunk_twist(twist, chunks - 1),
                 jnp.asarray(twist), turn, jnp.asarray(back), jnp.asarray(last)]
    whole = lambda shape: pl.BlockSpec(shape, lambda i: (0,) * len(shape))
    tile = lambda rows, shape: pl.BlockSpec((rows,) + shape[1:], lambda i: (i, 0, 0))
    out_shape = (count * chunks,) + data.shape[1:]
    return pl.pallas_call(
        functools.partial(azimuth_kernel, outer),
        grid=(count // block,),
        in_specs=[whole(value.shape) for value in constants]
        + [tile(block * chunks, value.shape) for value in early] + [tile(block, data.shape)],
        out_specs=tile(block * chunks, out_shape),
        out_shape=jax.ShapeDtypeStruct(out_shape, BF16),
        compiler_params=pltpu.CompilerParams(
            dimension_semantics=("arbitrary",), vmem_limit_bytes=16 * 1024 * 1024),
        name="azimuth_stage",
    )(*constants, *early, data)


def shifted(block, distance):
    devices = range(lax.axis_size("band"))
    route = [(i - distance, i) for i in devices if i - distance in devices]
    return lax.ppermute(block, "band", route)


def body(echoes, range_phase, pulse_shift, bin_offset, doppler_phase):
    range_count = lax.axis_size("range")
    group_size = lax.axis_size("pulse") * range_count
    cells_local = echoes.shape[3]
    cell_count = cells_local * range_count
    n_local = echoes.shape[2] // range_count
    spill_len = 2 * MARGIN
    owned_bins = cell_count - spill_len
    bins_local = owned_bins // group_size
    outer = cell_count // LANES
    sub = CHUNKS
    piece = n_local // sub
    steps = outer // sub

    band = lax.axis_index("band")
    bands = bin_offset.shape[0]
    order = jnp.arange(bands, dtype=jnp.int32)
    offset_of = lambda index: jnp.sum(jnp.where(order == index, bin_offset, 0))
    offset = offset_of(band)
    below = offset_of(band - 1)
    above = offset_of(band + 1)
    shift = offset - spill_len

    place = lax.axis_index("range")
    low = jnp.arange(outer, dtype=jnp.int32)
    lane = jnp.arange(LANES, dtype=jnp.int32)
    phase = jnp.concatenate((range_phase[0], range_phase[0]))
    phase = lax.dynamic_slice_in_dim(phase, spill_len - offset, cell_count, 0)
    phase = lax.optimization_barrier(jnp.transpose(phase.reshape(LANES, outer)))
    scale = 1.0 / math.sqrt(cell_count)
    phase = phase.reshape(steps, sub, LANES)
    part = lane // piece
    cube = (steps, LANES, LANES)
    spread = []
    for value in (jnp.cos(phase) * scale, jnp.sin(phase) * scale):
        wide = jnp.broadcast_to(value[:, sub - 1][..., None], cube)
        for h in range(sub - 1):
            wide = jnp.where(part == h, value[:, h][..., None], wide)
        spread.append(wide)
    spread = jnp.stack(spread)
    low_bin = jnp.arange(steps, dtype=jnp.int32)[:, None] * sub + part - shift

    def ramp(product):
        angle = jnp.mod(product, cell_count).astype(F32) * (-2.0 * math.pi / cell_count)
        return jnp.stack((jnp.cos(angle), jnp.sin(angle)))

    doppler = jnp.transpose(doppler_phase.reshape(LANES, group_size))
    factor = 1.0 / doppler_phase.shape[0]
    turn = jnp.stack((jnp.cos(doppler) * factor, jnp.sin(doppler) * factor))

    received = []
    source = echoes[0]
    for q in range(sub):
        blocks = []
        for d in range(range_count - 1, 0, -1):
            begin = jnp.mod(place + d, range_count) * n_local + q * piece
            block = lax.dynamic_slice_in_dim(source, begin, piece, 1)
            route = [(i, (i + d) % range_count) for i in range(range_count)]
            blocks.append(lax.ppermute(block, "range", route))
            if d == 1:
                source = lax.optimization_barrier(source)
        received.append(blocks)
    held = echoes[0].reshape(2, range_count, sub, piece, cells_local)
    scalars = jnp.stack((shift, place, below, above))

    twist = ramp((low[:, None] - shift) * (lane[None, :] + cells_local * place))
    samples = []
    gate = None
    for q in range(sub):
        shifts = jnp.tile(pulse_shift[0, q * piece:(q + 1) * piece], sub)
        near = ramp(low_bin * shifts)
        far = ramp(outer * lane[:, None] * shifts)
        gate = twist if gate is None else gate
        first = owned_bins // outer
        data, spill = cells_stage(scalars, held, q, received[q], twist, near, far, spread,
                                  gate, sub, first)
        own = owned_stage(data, near, far, spread, first)
        from_below = shifted(spill, 1)
        from_above = shifted(spill, -1)
        gate = stitch(scalars, own, from_below, from_above, sub,
                      group_size // range_count, range_count)
        blocks = gate.reshape(group_size, bins_local // sub, 2, LANES)
        block = lax.all_to_all(
            blocks, ("range", "pulse"), split_axis=0, concat_axis=0, tiled=True)
        samples.append(jnp.transpose(block, (1, 0, 2, 3)).reshape(
            bins_local // sub, 2 * group_size, LANES))

    early = [spread_stage(samples[q], q, group_size, range_count) for q in range(sub - 1)]
    image = azimuth_stage(early, samples[-1], turn, group_size, range_count)
    image = jnp.transpose(image.reshape(bins_local, group_size, 2, LANES), (0, 2, 1, 3))
    return image.reshape(bins_local, 2, group_size * LANES)


def solution(mesh):
    in_specs = (
        P("band", None, "pulse", "range"),
        P("band", None),
        P("band", ("pulse", "range")),
        P(),
        P(),
    )
    out_specs = P(("band", "pulse", "range"), None, None)
    return jax.shard_map(
        body, mesh=mesh, in_specs=in_specs, out_specs=out_specs, check_vma=False)
```

```python
import functools
import math

import jax
import jax.numpy as jnp
import ml_dtypes
import numpy as np
from jax import lax
from jax.experimental import pallas as pl
from jax.experimental.pallas import tpu as pltpu
from jax.sharding import PartitionSpec as P


MARGIN = 512
LANES = 128
CHUNKS = 2
F32 = jnp.float32
BF16 = jnp.bfloat16


def split_const(table):
    high = table.astype(ml_dtypes.bfloat16)
    low = (table - high.astype(np.float64)).astype(ml_dtypes.bfloat16)
    return high, low


def unit_roots(rows, cols, modulus, sign):
    product = np.outer(np.arange(rows), np.arange(cols)) % modulus
    angle = sign * 2.0 * np.pi * product / modulus
    return np.cos(angle), np.sin(angle)


def split_value(value):
    high = value.astype(BF16)
    low = (value - high.astype(F32)).astype(BF16)
    return high, low


def dot_f32(lhs, rhs, contract):
    return lax.dot_general(lhs, rhs, (contract, ((), ())), preferred_element_type=F32)


def complex_mul(a, b):
    return a[0] * b[0] - a[1] * b[1], a[0] * b[1] + a[1] * b[0]


def by_constant(a, angle):
    cos = math.cos(angle)
    sin = math.sin(angle)
    quarter = angle / (math.pi / 2)
    if abs(quarter - round(quarter)) < 1e-9:
        turn = int(round(quarter)) % 4
        if turn == 0:
            return a
        if turn == 1:
            return -a[1], a[0]
        if turn == 2:
            return -a[0], -a[1]
        return a[1], -a[0]
    if abs(abs(cos) - abs(sin)) < 1e-9:
        half = math.sqrt(0.5)
        plus = (a[0] + a[1]) * half
        minus = (a[0] - a[1]) * half
        if cos > 0 and sin > 0:
            return minus, plus
        if cos < 0 and sin > 0:
            return -plus, minus
        if cos < 0 and sin < 0:
            return -minus, -plus
        return plus, -minus
    return a[0] * cos - a[1] * sin, a[0] * sin + a[1] * cos


def small_dft(values, sign):
    count = len(values)
    if count == 1:
        return values
    even = small_dft(values[0::2], sign)
    odd = small_dft(values[1::2], sign)
    first = []
    second = []
    for i in range(count // 2):
        turned = by_constant(odd[i], sign * 2.0 * math.pi * i / count)
        first.append((even[i][0] + turned[0], even[i][1] + turned[1]))
        second.append((even[i][0] - turned[0], even[i][1] - turned[1]))
    return first + second


def bin_rows(table_ref, high, low):
    span = table_ref.shape[0] // 2
    product = dot_f32(table_ref[...], high, ((1,), (1,)))
    return product[:span] + product[span:] + dot_f32(table_ref[:span], low, ((1,), (1,)))


def turned_rows(product, lanes, rows, at, near_ref, far_ref, phase_ref):
    span = rows.stop - rows.start
    total = product[:, lanes]
    near = (near_ref[0, at:at + 1, :], near_ref[1, at:at + 1, :])
    far = (far_ref[0, rows, :], far_ref[1, rows, :])
    phase = (phase_ref[0, at, rows, :], phase_ref[1, at, rows, :])
    return complex_mul((total[:span], total[span:]), complex_mul(complex_mul(far, near), phase))


def ordered_rows(out_ref, order_ref, width):
    pitch = width + 8
    for n in range(out_ref.shape[0] // width):
        out_ref[n * width:(n + 1) * width, :] = (
            order_ref[n * pitch:n * pitch + width, :].astype(BF16))


def cells_kernel(outer, sub, sources, first, scalar_ref, mine_ref, *refs):
    echo_refs = (mine_ref,) + refs[:sources - 1]
    (twist_ref, near_ref, far_ref, phase_ref, table_ref, _, data_ref, spill_ref,
     stage_ref, mid_ref, order_ref) = refs[sources - 1:]
    rows = echo_refs[0].shape[1]
    inner = outer // sources
    group = 16

    def block(t, carry):
        at = pl.multiple_of(t * group, group)
        for n in range(inner):
            lanes = slice(n * LANES, (n + 1) * LANES)
            values = []
            for echo_ref in echo_refs:
                values.append((
                    echo_ref[0, pl.ds(at, group), lanes].astype(F32),
                    echo_ref[1, pl.ds(at, group), lanes].astype(F32),
                ))
            for q, value in enumerate(small_dft(values, -1.0)):
                value = by_constant(value, -2.0 * math.pi * n * q / outer)
                mid_ref[q, n, 0] = value[0]
                mid_ref[q, n, 1] = value[1]
        for q in range(sources):
            values = [(mid_ref[q, n, 0], mid_ref[q, n, 1]) for n in range(inner)]
            for m, value in enumerate(small_dft(values, -1.0)):
                stage_ref[q + sources * m, 0, pl.ds(at, group), :] = value[0]
                stage_ref[q + sources * m, 1, pl.ds(at, group), :] = value[1]
        return carry

    lax.fori_loop(0, rows // group, block, 0)
    shift = scalar_ref[0]
    steps = outer // sub
    pitch = 2 * steps + 8
    kept = slice(first, LANES)
    count = LANES - first
    for step in range(0, steps, 2):
        parts = []
        for i in range(2):
            halves = []
            for h in range(sub):
                bin_low = (step + i) * sub + h
                source = lax.rem(bin_low - shift + 2 * outer, outer)
                twist = (twist_ref[0, bin_low:bin_low + 1, :], twist_ref[1, bin_low:bin_low + 1, :])
                value = complex_mul((stage_ref[source, 0], stage_ref[source, 1]), twist)
                halves.append(jnp.concatenate(value, axis=1))
            part = split_value(jnp.concatenate(halves, axis=0))
            data_ref[0, step + i] = part[0]
            data_ref[1, step + i] = part[1]
            parts.append(part)
        product = bin_rows(table_ref, jnp.concatenate([part[0] for part in parts], axis=0),
                           jnp.concatenate([part[1] for part in parts], axis=0))
        for i in range(2):
            at = step + i
            lanes = slice(i * LANES, (i + 1) * LANES)
            value = turned_rows(product, lanes, kept, at, near_ref, far_ref, phase_ref)
            order_ref[pl.ds(2 * at, count, stride=pitch), :] = value[0]
            order_ref[pl.ds(2 * at + 1, count, stride=pitch), :] = value[1]
    ordered_rows(spill_ref, order_ref, 2 * steps)


def owned_kernel(data_ref, near_ref, far_ref, phase_ref, table_ref, out_ref, order_ref):
    steps = data_ref.shape[1]
    pitch = 2 * steps + 8
    count = table_ref.shape[0] // 4
    kept = slice(0, count)
    for step in range(0, steps, 2):
        product = bin_rows(table_ref, *[
            jnp.concatenate((data_ref[n, step], data_ref[n, step + 1]), axis=0) for n in range(2)])
        for i in range(2):
            at = step + i
            lanes = slice(i * LANES, (i + 1) * LANES)
            value = turned_rows(product, lanes, kept, at, near_ref, far_ref, phase_ref)
            order_ref[pl.ds(2 * at, count, stride=pitch), :] = value[0]
            order_ref[pl.ds(2 * at + 1, count, stride=pitch), :] = value[1]
    ordered_rows(out_ref, order_ref, 2 * steps)


def range_tables(first):
    cos, sin = unit_roots(LANES, LANES, LANES, -1.0)
    table = np.zeros((2, LANES, 2, LANES))
    table[0, :, 0], table[0, :, 1] = cos, -sin
    table[1, :, 0], table[1, :, 1] = sin, cos
    stack = lambda part: np.concatenate(split_const(part.reshape(-1, 2 * LANES)))
    return stack(table[:, :first]), stack(table[:, first:])


def cells_stage(scalars, echoes, chunk, received, twist, near, far, phase, gate, sub, first):
    sources = len(received) + 1
    outer = twist.shape[1]
    steps = outer // sub
    table = jnp.asarray(range_tables(first)[1])
    rows = echoes.shape[3]
    whole = lambda shape: pl.BlockSpec(shape, lambda i, s: (0,) * len(shape))
    mine = pl.BlockSpec((2, None, None) + echoes.shape[3:], lambda i, s: (0, s[1], chunk, 0, 0))
    operands = (*received, twist, near, far, phase, table)
    data = jax.ShapeDtypeStruct((2, steps, LANES, 2 * LANES), BF16)
    spill = jax.ShapeDtypeStruct((2 * steps * (LANES - first), LANES), BF16)
    return pl.pallas_call(
        functools.partial(cells_kernel, outer, sub, sources, first),
        grid_spec=pltpu.PrefetchScalarGridSpec(
            num_scalar_prefetch=1,
            grid=(1,),
            in_specs=[mine, *[whole(value.shape) for value in operands],
                      pl.BlockSpec(memory_space=pl.ANY)],
            out_specs=[whole(data.shape), whole(spill.shape)],
            scratch_shapes=[
                pltpu.VMEM((outer, 2, rows, LANES), F32),
                pltpu.VMEM((sources, outer // sources, 2, 16, LANES), F32),
                pltpu.VMEM(((LANES - first) * (2 * steps + 8), LANES), F32),
            ],
        ),
        out_shape=[data, spill],
        compiler_params=pltpu.CompilerParams(
            dimension_semantics=("arbitrary",), vmem_limit_bytes=16 * 1024 * 1024),
        name="cells_stage",
    )(scalars, echoes, *operands, gate)


def owned_stage(data, near, far, phase, first):
    steps = data.shape[1]
    table = jnp.asarray(range_tables(first)[0])
    vmem = pl.BlockSpec(memory_space=pltpu.VMEM)
    return pl.pallas_call(
        owned_kernel,
        in_specs=[vmem] * 5,
        out_specs=vmem,
        out_shape=jax.ShapeDtypeStruct((2 * steps * first, LANES), BF16),
        scratch_shapes=[pltpu.VMEM((first * (2 * steps + 8), LANES), F32)],
        compiler_params=pltpu.CompilerParams(vmem_limit_bytes=12 * 1024 * 1024),
        name="owned_stage",
    )(data, near, far, phase, table)


def stitch_kernel(sub, scalar_ref, own_ref, low_ref, high_ref, out_ref, held_ref, sems):
    _, ranges, height, _ = held_ref.shape
    unit = 16
    edge = low_ref.shape[0] // unit
    count = own_ref.shape[0] // unit
    per_block = height // unit
    lane = lax.broadcasted_iota(jnp.int32, (unit, LANES), 1)
    row = lax.broadcasted_iota(jnp.int32, (unit, LANES), 0)
    index = row // 2 * sub + lane // (LANES // sub)
    per_unit = unit // 2 * sub
    for i in range(count):
        rows = slice(i * unit, (i + 1) * unit)
        value = own_ref[rows]
        if i < edge:
            added = jnp.where(index < scalar_ref[2] - i * per_unit, low_ref[rows].astype(F32), 0.0)
            value = (value.astype(F32) + added).astype(BF16)
        elif i >= count - edge:
            j = i - (count - edge)
            other = high_ref[j * unit:(j + 1) * unit].astype(F32)
            added = jnp.where(index >= scalar_ref[3] - j * per_unit, other, 0.0)
            value = (value.astype(F32) + added).astype(BF16)
        block = i // per_block
        at = i % per_block * unit
        held_ref[block // ranges, block % ranges, at:at + unit] = value
    copies = [pltpu.make_async_copy(held_ref.at[:, r], out_ref.at[r], sems.at[r])
              for r in range(ranges)]
    for copy in copies:
        copy.start()
    for copy in copies:
        copy.wait()


def stitch(scalars, own, from_below, from_above, sub, pulses, ranges):
    vmem = pl.BlockSpec(memory_space=pltpu.VMEM)
    height = own.shape[0] // (pulses * ranges)
    return pl.pallas_call(
        functools.partial(stitch_kernel, sub),
        in_specs=[pl.BlockSpec(memory_space=pltpu.SMEM), vmem, vmem, vmem],
        out_specs=pl.BlockSpec(memory_space=pl.ANY),
        out_shape=jax.ShapeDtypeStruct((ranges, pulses, height, LANES), BF16),
        scratch_shapes=[pltpu.VMEM((pulses, ranges, height, LANES), BF16),
                        pltpu.SemaphoreType.DMA((ranges,))],
        compiler_params=pltpu.CompilerParams(vmem_limit_bytes=8 * 1024 * 1024),
        name="stitch",
    )(scalars, own, from_below, from_above)


def spread_rows(first_ref, data, twist_ref):
    left = ((1,), (0,))
    wide = jnp.concatenate(data, axis=1)
    spread = dot_f32(first_ref[0], wide, left) + dot_f32(first_ref[1], wide, left)
    half = spread.shape[0] // 2
    twist = (twist_ref[0], twist_ref[1])
    rows = []
    for i in range(len(data)):
        lanes = slice(i * LANES, (i + 1) * LANES)
        real, imag = complex_mul((spread[:half, lanes], spread[half:, lanes]), twist)
        width = LANES // CHUNKS
        for h in range(CHUNKS):
            part = slice(h * width, (h + 1) * width)
            rows.append(jnp.concatenate((real[:, part], imag[:, part]), axis=1).astype(BF16))
    return rows


def spread_kernel(first_ref, twist_ref, data_ref, out_ref):
    for c in range(0, data_ref.shape[0], 2):
        rows = spread_rows(first_ref, (data_ref[c], data_ref[c + 1]), twist_ref)
        for i, value in enumerate(rows):
            out_ref[c * CHUNKS + i] = value


def azimuth_kernel(outer, first_ref, fore_ref, twist_ref, back_twist_ref, filter_ref, back_ref,
                   last_ref, *refs):
    early_refs = refs[:-2]
    data_ref, out_ref = refs[-2:]
    twist_back = (back_twist_ref[0], -back_twist_ref[1])
    turn = (filter_ref[0], filter_ref[1])
    left = ((1,), (0,))
    two = lambda lhs, rhs: dot_f32(lhs[0], rhs, left) + dot_f32(lhs[1], rhs, left)
    rows = []
    for c in range(0, data_ref.shape[0], 2):
        rows += spread_rows(first_ref, (data_ref[c], data_ref[c + 1]), twist_ref)
    total = len(rows)
    rows = [jnp.concatenate([ref[c] for ref in early_refs] + [rows[c]], axis=1)
            for c in range(total)]
    stacked = jnp.concatenate(rows, axis=0)
    doppler = dot_f32(stacked, fore_ref[...], left)
    rows = []
    for c in range(total):
        part = doppler[c * outer:(c + 1) * outer]
        value = complex_mul((part[:, :LANES], part[:, LANES:]), turn)
        rows.append(jnp.concatenate(value, axis=1).astype(BF16))
    stacked = jnp.concatenate(rows, axis=0)
    image = dot_f32(stacked, back_ref[...], left)
    for c in range(0, total, 2):
        values = []
        for d in range(2):
            part = image[(c + d) * outer:(c + d + 1) * outer]
            value = complex_mul((part[:, :LANES], part[:, LANES:]), twist_back)
            values.append(jnp.concatenate(value, axis=0).astype(BF16))
        value = two((last_ref[0], last_ref[1]), jnp.concatenate(values, axis=1)).astype(BF16)
        out_ref[c] = value[:, :LANES]
        out_ref[c + 1] = value[:, LANES:]


def azimuth_tables(outer, ranges):
    cos, sin = unit_roots(outer, outer, outer, -1.0)
    first = np.zeros((2, outer, outer, 2))
    first[0, :, :, 0], first[0, :, :, 1] = cos, -sin
    first[1, :, :, 0], first[1, :, :, 1] = sin, cos
    slots = np.arange(outer)
    first = first[:, :, slots % (outer // ranges) * ranges + slots // (outer // ranges)]
    last = np.zeros((outer, 2, 2, outer))
    last[:, 0, 0], last[:, 0, 1] = cos, sin
    last[:, 1, 0], last[:, 1, 1] = -sin, cos
    cos, sin = unit_roots(LANES, LANES, LANES, -1.0)
    fore = np.zeros((2, LANES, 2, LANES))
    fore[0, :, 0], fore[0, :, 1] = cos, sin
    fore[1, :, 0], fore[1, :, 1] = -sin, cos
    back = np.zeros((2, LANES, 2, LANES))
    back[0, :, 0], back[0, :, 1] = cos, -sin
    back[1, :, 0], back[1, :, 1] = sin, cos
    pair = lambda table, shape: np.stack(split_const(table.reshape(shape)))
    fore = fore.reshape(2, CHUNKS, LANES // CHUNKS, 2 * LANES).transpose(1, 0, 2, 3)
    twist = np.stack(unit_roots(outer, LANES, outer * LANES, -1.0)).astype(np.float32)
    square = (2 * LANES, 2 * LANES)
    side = (2 * outer, 2 * outer)
    half = lambda table: table.reshape(square).astype(ml_dtypes.bfloat16)
    return pair(first, side), half(fore), twist, half(back), pair(last, side)


def chunk_twist(twist, chunk):
    width = LANES // CHUNKS
    return jnp.asarray(np.tile(twist[:, :, chunk * width:(chunk + 1) * width], CHUNKS))


def spread_stage(data, chunk, outer, ranges):
    first, _, twist, _, _ = azimuth_tables(outer, ranges)
    vmem = pl.BlockSpec(memory_space=pltpu.VMEM)
    return pl.pallas_call(
        spread_kernel,
        in_specs=[vmem] * 3,
        out_specs=vmem,
        out_shape=jax.ShapeDtypeStruct((data.shape[0] * CHUNKS, outer, LANES), BF16),
        compiler_params=pltpu.CompilerParams(vmem_limit_bytes=12 * 1024 * 1024),
        name="spread_stage",
    )(jnp.asarray(first), chunk_twist(twist, chunk), data)


def azimuth_stage(early, data, turn, outer, ranges):
    chunks = CHUNKS
    count = data.shape[0]
    block = 24 // chunks
    first, fore, twist, back, last = azimuth_tables(outer, ranges)
    constants = [jnp.asarray(first), jnp.asarray(fore), chunk_twist(twist, chunks - 1),
                 jnp.asarray(twist), turn, jnp.asarray(back), jnp.asarray(last)]
    whole = lambda shape: pl.BlockSpec(shape, lambda i: (0,) * len(shape))
    tile = lambda rows, shape: pl.BlockSpec((rows,) + shape[1:], lambda i: (i, 0, 0))
    out_shape = (count * chunks,) + data.shape[1:]
    return pl.pallas_call(
        functools.partial(azimuth_kernel, outer),
        grid=(count // block,),
        in_specs=[whole(value.shape) for value in constants]
        + [tile(block * chunks, value.shape) for value in early] + [tile(block, data.shape)],
        out_specs=tile(block * chunks, out_shape),
        out_shape=jax.ShapeDtypeStruct(out_shape, BF16),
        compiler_params=pltpu.CompilerParams(
            dimension_semantics=("arbitrary",), vmem_limit_bytes=16 * 1024 * 1024),
        name="azimuth_stage",
    )(*constants, *early, data)


def shifted(block, distance):
    devices = range(lax.axis_size("band"))
    route = [(i - distance, i) for i in devices if i - distance in devices]
    return lax.ppermute(block, "band", route)


def body(echoes, range_phase, pulse_shift, bin_offset, doppler_phase):
    range_count = lax.axis_size("range")
    group_size = lax.axis_size("pulse") * range_count
    cells_local = echoes.shape[3]
    cell_count = cells_local * range_count
    n_local = echoes.shape[2] // range_count
    spill_len = 2 * MARGIN
    owned_bins = cell_count - spill_len
    bins_local = owned_bins // group_size
    outer = cell_count // LANES
    sub = CHUNKS
    piece = n_local // sub
    steps = outer // sub

    band = lax.axis_index("band")
    bands = bin_offset.shape[0]
    order = jnp.arange(bands, dtype=jnp.int32)
    offset_of = lambda index: jnp.sum(jnp.where(order == index, bin_offset, 0))
    offset = offset_of(band)
    below = offset_of(band - 1)
    above = offset_of(band + 1)
    shift = offset - spill_len

    place = lax.axis_index("range")
    low = jnp.arange(outer, dtype=jnp.int32)
    lane = jnp.arange(LANES, dtype=jnp.int32)
    phase = jnp.concatenate((range_phase[0], range_phase[0]))
    phase = lax.dynamic_slice_in_dim(phase, spill_len - offset, cell_count, 0)
    phase = lax.optimization_barrier(jnp.transpose(phase.reshape(LANES, outer)))
    scale = 1.0 / math.sqrt(cell_count)
    phase = phase.reshape(steps, sub, LANES)
    part = lane // piece
    cube = (steps, LANES, LANES)
    spread = []
    for value in (jnp.cos(phase) * scale, jnp.sin(phase) * scale):
        wide = jnp.broadcast_to(value[:, sub - 1][..., None], cube)
        for h in range(sub - 1):
            wide = jnp.where(part == h, value[:, h][..., None], wide)
        spread.append(wide)
    spread = jnp.stack(spread)
    low_bin = jnp.arange(steps, dtype=jnp.int32)[:, None] * sub + part - shift

    def ramp(product):
        angle = jnp.mod(product, cell_count).astype(F32) * (-2.0 * math.pi / cell_count)
        return jnp.stack((jnp.cos(angle), jnp.sin(angle)))

    doppler = jnp.transpose(doppler_phase.reshape(LANES, group_size))
    factor = 1.0 / doppler_phase.shape[0]
    turn = jnp.stack((jnp.cos(doppler) * factor, jnp.sin(doppler) * factor))

    received = []
    source = echoes[0]
    for q in range(sub):
        blocks = []
        for d in range(range_count - 1, 0, -1):
            begin = jnp.mod(place + d, range_count) * n_local + q * piece
            block = lax.dynamic_slice_in_dim(source, begin, piece, 1)
            route = [(i, (i + d) % range_count) for i in range(range_count)]
            blocks.append(lax.ppermute(block, "range", route))
            if d == 1:
                source = lax.optimization_barrier(source)
        received.append(blocks)
    held = echoes[0].reshape(2, range_count, sub, piece, cells_local)
    scalars = jnp.stack((shift, place, below, above))

    twist = ramp((low[:, None] - shift) * (lane[None, :] + cells_local * place))
    samples = []
    gate = None
    for q in range(sub):
        shifts = jnp.tile(pulse_shift[0, q * piece:(q + 1) * piece], sub)
        near = ramp(low_bin * shifts)
        far = ramp(outer * lane[:, None] * shifts)
        gate = twist if gate is None else gate
        first = owned_bins // outer
        data, spill = cells_stage(scalars, held, q, received[q], twist, near, far, spread,
                                  gate, sub, first)
        own = owned_stage(data, near, far, spread, first)
        from_below = shifted(spill, 1)
        from_above = shifted(spill, -1)
        gate = stitch(scalars, own, from_below, from_above, sub,
                      group_size // range_count, range_count)
        blocks = gate.reshape(group_size, bins_local // sub, 2, LANES)
        block = lax.all_to_all(
            blocks, ("range", "pulse"), split_axis=0, concat_axis=0, tiled=True)
        samples.append(jnp.transpose(block, (1, 0, 2, 3)).reshape(
            bins_local // sub, 2 * group_size, LANES))

    early = [spread_stage(samples[q], q, group_size, range_count) for q in range(sub - 1)]
    image = azimuth_stage(early, samples[-1], turn, group_size, range_count)
    image = jnp.transpose(image.reshape(bins_local, group_size, 2, LANES), (0, 2, 1, 3))
    return image.reshape(bins_local, 2, group_size * LANES)


def solution(mesh):
    in_specs = (
        P("band", None, "pulse", "range"),
        P("band", None),
        P("band", ("pulse", "range")),
        P(),
        P(),
    )
    out_specs = P(("band", "pulse", "range"), None, None)
    return jax.shard_map(
        body, mesh=mesh, in_specs=in_specs, out_specs=out_specs, check_vma=False)
```

```python
import functools
import math

import jax
import jax.numpy as jnp
import ml_dtypes
import numpy as np
from jax import lax
from jax.experimental import pallas as pl
from jax.experimental.pallas import tpu as pltpu
from jax.sharding import PartitionSpec as P


MARGIN = 512
LANES = 128
CHUNKS = 2
F32 = jnp.float32
BF16 = jnp.bfloat16


def split_const(table):
    high = table.astype(ml_dtypes.bfloat16)
    low = (table - high.astype(np.float64)).astype(ml_dtypes.bfloat16)
    return high, low


def unit_roots(rows, cols, modulus, sign):
    product = np.outer(np.arange(rows), np.arange(cols)) % modulus
    angle = sign * 2.0 * np.pi * product / modulus
    return np.cos(angle), np.sin(angle)


def split_value(value):
    high = value.astype(BF16)
    low = (value - high.astype(F32)).astype(BF16)
    return high, low


def dot_f32(lhs, rhs, contract):
    return lax.dot_general(lhs, rhs, (contract, ((), ())), preferred_element_type=F32)


def complex_mul(a, b):
    return a[0] * b[0] - a[1] * b[1], a[0] * b[1] + a[1] * b[0]


def by_constant(a, angle):
    cos = math.cos(angle)
    sin = math.sin(angle)
    quarter = angle / (math.pi / 2)
    if abs(quarter - round(quarter)) < 1e-9:
        turn = int(round(quarter)) % 4
        if turn == 0:
            return a
        if turn == 1:
            return -a[1], a[0]
        if turn == 2:
            return -a[0], -a[1]
        return a[1], -a[0]
    if abs(abs(cos) - abs(sin)) < 1e-9:
        half = math.sqrt(0.5)
        plus = (a[0] + a[1]) * half
        minus = (a[0] - a[1]) * half
        if cos > 0 and sin > 0:
            return minus, plus
        if cos < 0 and sin > 0:
            return -plus, minus
        if cos < 0 and sin < 0:
            return -minus, -plus
        return plus, -minus
    return a[0] * cos - a[1] * sin, a[0] * sin + a[1] * cos


def small_dft(values, sign):
    count = len(values)
    if count == 1:
        return values
    even = small_dft(values[0::2], sign)
    odd = small_dft(values[1::2], sign)
    first = []
    second = []
    for i in range(count // 2):
        turned = by_constant(odd[i], sign * 2.0 * math.pi * i / count)
        first.append((even[i][0] + turned[0], even[i][1] + turned[1]))
        second.append((even[i][0] - turned[0], even[i][1] - turned[1]))
    return first + second


def bin_rows(table_ref, high, low):
    span = table_ref.shape[0] // 2
    product = dot_f32(table_ref[...], high, ((1,), (1,)))
    return product[:span] + product[span:] + dot_f32(table_ref[:span], low, ((1,), (1,)))


def turned_rows(product, lanes, rows, at, near_ref, far_ref, phase_ref):
    span = rows.stop - rows.start
    total = product[:, lanes]
    near = (near_ref[0, at:at + 1, :], near_ref[1, at:at + 1, :])
    far = (far_ref[0, rows, :], far_ref[1, rows, :])
    phase = (phase_ref[0, at, rows, :], phase_ref[1, at, rows, :])
    return complex_mul((total[:span], total[span:]), complex_mul(complex_mul(far, near), phase))


def ordered_rows(out_ref, order_ref, width):
    pitch = width + 8
    for n in range(out_ref.shape[0] // width):
        out_ref[n * width:(n + 1) * width, :] = (
            order_ref[n * pitch:n * pitch + width, :].astype(BF16))


def cells_kernel(outer, sub, sources, first, scalar_ref, mine_ref, *refs):
    echo_refs = (mine_ref,) + refs[:sources - 1]
    (twist_ref, near_ref, far_ref, phase_ref, table_ref, _, data_ref, spill_ref,
     stage_ref, mid_ref, order_ref) = refs[sources - 1:]
    rows = echo_refs[0].shape[1]
    inner = outer // sources
    group = 16

    def block(t, carry):
        at = pl.multiple_of(t * group, group)
        for n in range(inner):
            lanes = slice(n * LANES, (n + 1) * LANES)
            values = []
            for echo_ref in echo_refs:
                values.append((
                    echo_ref[0, pl.ds(at, group), lanes].astype(F32),
                    echo_ref[1, pl.ds(at, group), lanes].astype(F32),
                ))
            for q, value in enumerate(small_dft(values, -1.0)):
                value = by_constant(value, -2.0 * math.pi * n * q / outer)
                mid_ref[q, n, 0] = value[0]
                mid_ref[q, n, 1] = value[1]
        for q in range(sources):
            values = [(mid_ref[q, n, 0], mid_ref[q, n, 1]) for n in range(inner)]
            for m, value in enumerate(small_dft(values, -1.0)):
                stage_ref[q + sources * m, 0, pl.ds(at, group), :] = value[0]
                stage_ref[q + sources * m, 1, pl.ds(at, group), :] = value[1]
        return carry

    lax.fori_loop(0, rows // group, block, 0)
    shift = scalar_ref[0]
    steps = outer // sub
    pitch = 2 * steps + 8
    kept = slice(first, LANES)
    count = LANES - first
    for step in range(0, steps, 2):
        parts = []
        for i in range(2):
            halves = []
            for h in range(sub):
                bin_low = (step + i) * sub + h
                source = lax.rem(bin_low - shift + 2 * outer, outer)
                twist = (twist_ref[0, bin_low:bin_low + 1, :], twist_ref[1, bin_low:bin_low + 1, :])
                value = complex_mul((stage_ref[source, 0], stage_ref[source, 1]), twist)
                halves.append(jnp.concatenate(value, axis=1))
            part = split_value(jnp.concatenate(halves, axis=0))
            data_ref[0, step + i] = part[0]
            data_ref[1, step + i] = part[1]
            parts.append(part)
        product = bin_rows(table_ref, jnp.concatenate([part[0] for part in parts], axis=0),
                           jnp.concatenate([part[1] for part in parts], axis=0))
        for i in range(2):
            at = step + i
            lanes = slice(i * LANES, (i + 1) * LANES)
            value = turned_rows(product, lanes, kept, at, near_ref, far_ref, phase_ref)
            order_ref[pl.ds(2 * at, count, stride=pitch), :] = value[0]
            order_ref[pl.ds(2 * at + 1, count, stride=pitch), :] = value[1]
    ordered_rows(spill_ref, order_ref, 2 * steps)


def owned_kernel(data_ref, near_ref, far_ref, phase_ref, table_ref, out_ref, order_ref):
    steps = data_ref.shape[1]
    pitch = 2 * steps + 8
    count = table_ref.shape[0] // 4
    kept = slice(0, count)
    for step in range(0, steps, 2):
        product = bin_rows(table_ref, *[
            jnp.concatenate((data_ref[n, step], data_ref[n, step + 1]), axis=0) for n in range(2)])
        for i in range(2):
            at = step + i
            lanes = slice(i * LANES, (i + 1) * LANES)
            value = turned_rows(product, lanes, kept, at, near_ref, far_ref, phase_ref)
            order_ref[pl.ds(2 * at, count, stride=pitch), :] = value[0]
            order_ref[pl.ds(2 * at + 1, count, stride=pitch), :] = value[1]
    ordered_rows(out_ref, order_ref, 2 * steps)


def range_tables(first):
    cos, sin = unit_roots(LANES, LANES, LANES, -1.0)
    table = np.zeros((2, LANES, 2, LANES))
    table[0, :, 0], table[0, :, 1] = cos, -sin
    table[1, :, 0], table[1, :, 1] = sin, cos
    stack = lambda part: np.concatenate(split_const(part.reshape(-1, 2 * LANES)))
    return stack(table[:, :first]), stack(table[:, first:])


def cells_stage(scalars, echoes, chunk, received, twist, near, far, phase, gate, sub, first):
    sources = len(received) + 1
    outer = twist.shape[1]
    steps = outer // sub
    table = jnp.asarray(range_tables(first)[1])
    rows = echoes.shape[3]
    whole = lambda shape: pl.BlockSpec(shape, lambda i, s: (0,) * len(shape))
    mine = pl.BlockSpec((2, None, None) + echoes.shape[3:], lambda i, s: (0, s[1], chunk, 0, 0))
    operands = (*received, twist, near, far, phase, table)
    data = jax.ShapeDtypeStruct((2, steps, LANES, 2 * LANES), BF16)
    spill = jax.ShapeDtypeStruct((2 * steps * (LANES - first), LANES), BF16)
    return pl.pallas_call(
        functools.partial(cells_kernel, outer, sub, sources, first),
        grid_spec=pltpu.PrefetchScalarGridSpec(
            num_scalar_prefetch=1,
            grid=(1,),
            in_specs=[mine, *[whole(value.shape) for value in operands],
                      pl.BlockSpec(memory_space=pl.ANY)],
            out_specs=[whole(data.shape), whole(spill.shape)],
            scratch_shapes=[
                pltpu.VMEM((outer, 2, rows, LANES), F32),
                pltpu.VMEM((sources, outer // sources, 2, 16, LANES), F32),
                pltpu.VMEM(((LANES - first) * (2 * steps + 8), LANES), F32),
            ],
        ),
        out_shape=[data, spill],
        compiler_params=pltpu.CompilerParams(
            dimension_semantics=("arbitrary",), vmem_limit_bytes=16 * 1024 * 1024),
        name="cells_stage",
    )(scalars, echoes, *operands, gate)


def owned_stage(data, near, far, phase, first):
    steps = data.shape[1]
    table = jnp.asarray(range_tables(first)[0])
    vmem = pl.BlockSpec(memory_space=pltpu.VMEM)
    return pl.pallas_call(
        owned_kernel,
        in_specs=[vmem] * 5,
        out_specs=vmem,
        out_shape=jax.ShapeDtypeStruct((2 * steps * first, LANES), BF16),
        scratch_shapes=[pltpu.VMEM((first * (2 * steps + 8), LANES), F32)],
        compiler_params=pltpu.CompilerParams(vmem_limit_bytes=12 * 1024 * 1024),
        name="owned_stage",
    )(data, near, far, phase, table)


def stitch_kernel(sub, scalar_ref, own_ref, low_ref, high_ref, out_ref, held_ref, sems):
    _, ranges, height, _ = held_ref.shape
    unit = 16
    edge = low_ref.shape[0] // unit
    count = own_ref.shape[0] // unit
    per_block = height // unit
    lane = lax.broadcasted_iota(jnp.int32, (unit, LANES), 1)
    row = lax.broadcasted_iota(jnp.int32, (unit, LANES), 0)
    index = row // 2 * sub + lane // (LANES // sub)
    per_unit = unit // 2 * sub
    for i in range(count):
        rows = slice(i * unit, (i + 1) * unit)
        value = own_ref[rows]
        if i < edge:
            added = jnp.where(index < scalar_ref[2] - i * per_unit, low_ref[rows].astype(F32), 0.0)
            value = (value.astype(F32) + added).astype(BF16)
        elif i >= count - edge:
            j = i - (count - edge)
            other = high_ref[j * unit:(j + 1) * unit].astype(F32)
            added = jnp.where(index >= scalar_ref[3] - j * per_unit, other, 0.0)
            value = (value.astype(F32) + added).astype(BF16)
        block = i // per_block
        at = i % per_block * unit
        held_ref[block // ranges, block % ranges, at:at + unit] = value
    copies = [pltpu.make_async_copy(held_ref.at[:, r], out_ref.at[r], sems.at[r])
              for r in range(ranges)]
    for copy in copies:
        copy.start()
    for copy in copies:
        copy.wait()


def stitch(scalars, own, from_below, from_above, sub, pulses, ranges):
    vmem = pl.BlockSpec(memory_space=pltpu.VMEM)
    height = own.shape[0] // (pulses * ranges)
    return pl.pallas_call(
        functools.partial(stitch_kernel, sub),
        in_specs=[pl.BlockSpec(memory_space=pltpu.SMEM), vmem, vmem, vmem],
        out_specs=pl.BlockSpec(memory_space=pl.ANY),
        out_shape=jax.ShapeDtypeStruct((ranges, pulses, height, LANES), BF16),
        scratch_shapes=[pltpu.VMEM((pulses, ranges, height, LANES), BF16),
                        pltpu.SemaphoreType.DMA((ranges,))],
        compiler_params=pltpu.CompilerParams(vmem_limit_bytes=8 * 1024 * 1024),
        name="stitch",
    )(scalars, own, from_below, from_above)


def spread_rows(first_ref, data, twist_ref):
    left = ((1,), (0,))
    wide = jnp.concatenate(data, axis=1)
    spread = dot_f32(first_ref[...], wide, left)
    half = spread.shape[0] // 2
    twist = (twist_ref[0], twist_ref[1])
    rows = []
    for i in range(len(data)):
        lanes = slice(i * LANES, (i + 1) * LANES)
        real, imag = complex_mul((spread[:half, lanes], spread[half:, lanes]), twist)
        width = LANES // CHUNKS
        for h in range(CHUNKS):
            part = slice(h * width, (h + 1) * width)
            rows.append(jnp.concatenate((real[:, part], imag[:, part]), axis=1).astype(BF16))
    return rows


def spread_kernel(first_ref, twist_ref, data_ref, out_ref):
    for c in range(0, data_ref.shape[0], 2):
        rows = spread_rows(first_ref, (data_ref[c], data_ref[c + 1]), twist_ref)
        for i, value in enumerate(rows):
            out_ref[c * CHUNKS + i] = value


def azimuth_kernel(outer, first_ref, fore_ref, twist_ref, back_twist_ref, filter_ref, back_ref,
                   last_ref, *refs):
    early_refs = refs[:-2]
    data_ref, out_ref = refs[-2:]
    twist_back = (back_twist_ref[0], -back_twist_ref[1])
    turn = (filter_ref[0], filter_ref[1])
    left = ((1,), (0,))
    rows = []
    for c in range(0, data_ref.shape[0], 2):
        rows += spread_rows(first_ref, (data_ref[c], data_ref[c + 1]), twist_ref)
    total = len(rows)
    rows = [jnp.concatenate([ref[c] for ref in early_refs] + [rows[c]], axis=1)
            for c in range(total)]
    stacked = jnp.concatenate(rows, axis=0)
    doppler = dot_f32(stacked, fore_ref[...], left)
    rows = []
    for c in range(total):
        part = doppler[c * outer:(c + 1) * outer]
        value = complex_mul((part[:, :LANES], part[:, LANES:]), turn)
        rows.append(jnp.concatenate(value, axis=1).astype(BF16))
    stacked = jnp.concatenate(rows, axis=0)
    image = dot_f32(stacked, back_ref[...], left)
    for c in range(0, total, 2):
        values = []
        for d in range(2):
            part = image[(c + d) * outer:(c + d + 1) * outer]
            value = complex_mul((part[:, :LANES], part[:, LANES:]), twist_back)
            values.append(jnp.concatenate(value, axis=0).astype(BF16))
        value = dot_f32(last_ref[...], jnp.concatenate(values, axis=1), left).astype(BF16)
        out_ref[c] = value[:, :LANES]
        out_ref[c + 1] = value[:, LANES:]


def azimuth_tables(outer, ranges):
    cos, sin = unit_roots(outer, outer, outer, -1.0)
    first = np.zeros((2, outer, outer, 2))
    first[0, :, :, 0], first[0, :, :, 1] = cos, -sin
    first[1, :, :, 0], first[1, :, :, 1] = sin, cos
    slots = np.arange(outer)
    first = first[:, :, slots % (outer // ranges) * ranges + slots // (outer // ranges)]
    last = np.zeros((outer, 2, 2, outer))
    last[:, 0, 0], last[:, 0, 1] = cos, sin
    last[:, 1, 0], last[:, 1, 1] = -sin, cos
    cos, sin = unit_roots(LANES, LANES, LANES, -1.0)
    fore = np.zeros((2, LANES, 2, LANES))
    fore[0, :, 0], fore[0, :, 1] = cos, sin
    fore[1, :, 0], fore[1, :, 1] = -sin, cos
    back = np.zeros((2, LANES, 2, LANES))
    back[0, :, 0], back[0, :, 1] = cos, -sin
    back[1, :, 0], back[1, :, 1] = sin, cos
    half = lambda table, shape: table.reshape(shape).astype(ml_dtypes.bfloat16)
    fore = fore.reshape(2, CHUNKS, LANES // CHUNKS, 2 * LANES).transpose(1, 0, 2, 3)
    twist = np.stack(unit_roots(outer, LANES, outer * LANES, -1.0)).astype(np.float32)
    square = (2 * LANES, 2 * LANES)
    side = (2 * outer, 2 * outer)
    return half(first, side), half(fore, square), twist, half(back, square), half(last, side)


def chunk_twist(twist, chunk):
    width = LANES // CHUNKS
    return jnp.asarray(np.tile(twist[:, :, chunk * width:(chunk + 1) * width], CHUNKS))


def spread_stage(data, chunk, outer, ranges):
    first, _, twist, _, _ = azimuth_tables(outer, ranges)
    vmem = pl.BlockSpec(memory_space=pltpu.VMEM)
    return pl.pallas_call(
        spread_kernel,
        in_specs=[vmem] * 3,
        out_specs=vmem,
        out_shape=jax.ShapeDtypeStruct((data.shape[0] * CHUNKS, outer, LANES), BF16),
        compiler_params=pltpu.CompilerParams(vmem_limit_bytes=12 * 1024 * 1024),
        name="spread_stage",
    )(jnp.asarray(first), chunk_twist(twist, chunk), data)


def azimuth_stage(early, data, turn, outer, ranges):
    chunks = CHUNKS
    count = data.shape[0]
    block = 24 // chunks
    first, fore, twist, back, last = azimuth_tables(outer, ranges)
    constants = [jnp.asarray(first), jnp.asarray(fore), chunk_twist(twist, chunks - 1),
                 jnp.asarray(twist), turn, jnp.asarray(back), jnp.asarray(last)]
    whole = lambda shape: pl.BlockSpec(shape, lambda i: (0,) * len(shape))
    tile = lambda rows, shape: pl.BlockSpec((rows,) + shape[1:], lambda i: (i, 0, 0))
    out_shape = (count * chunks,) + data.shape[1:]
    return pl.pallas_call(
        functools.partial(azimuth_kernel, outer),
        grid=(count // block,),
        in_specs=[whole(value.shape) for value in constants]
        + [tile(block * chunks, value.shape) for value in early] + [tile(block, data.shape)],
        out_specs=tile(block * chunks, out_shape),
        out_shape=jax.ShapeDtypeStruct(out_shape, BF16),
        compiler_params=pltpu.CompilerParams(
            dimension_semantics=("arbitrary",), vmem_limit_bytes=16 * 1024 * 1024),
        name="azimuth_stage",
    )(*constants, *early, data)


def shifted(block, distance):
    devices = range(lax.axis_size("band"))
    route = [(i - distance, i) for i in devices if i - distance in devices]
    return lax.ppermute(block, "band", route)


def body(echoes, range_phase, pulse_shift, bin_offset, doppler_phase):
    range_count = lax.axis_size("range")
    group_size = lax.axis_size("pulse") * range_count
    cells_local = echoes.shape[3]
    cell_count = cells_local * range_count
    n_local = echoes.shape[2] // range_count
    spill_len = 2 * MARGIN
    owned_bins = cell_count - spill_len
    bins_local = owned_bins // group_size
    outer = cell_count // LANES
    sub = CHUNKS
    piece = n_local // sub
    steps = outer // sub

    band = lax.axis_index("band")
    bands = bin_offset.shape[0]
    order = jnp.arange(bands, dtype=jnp.int32)
    offset_of = lambda index: jnp.sum(jnp.where(order == index, bin_offset, 0))
    offset = offset_of(band)
    below = offset_of(band - 1)
    above = offset_of(band + 1)
    shift = offset - spill_len

    place = lax.axis_index("range")
    low = jnp.arange(outer, dtype=jnp.int32)
    lane = jnp.arange(LANES, dtype=jnp.int32)
    phase = jnp.concatenate((range_phase[0], range_phase[0]))
    phase = lax.dynamic_slice_in_dim(phase, spill_len - offset, cell_count, 0)
    phase = lax.optimization_barrier(jnp.transpose(phase.reshape(LANES, outer)))
    scale = 1.0 / math.sqrt(cell_count)
    phase = phase.reshape(steps, sub, LANES)
    part = lane // piece
    cube = (steps, LANES, LANES)
    spread = []
    for value in (jnp.cos(phase) * scale, jnp.sin(phase) * scale):
        wide = jnp.broadcast_to(value[:, sub - 1][..., None], cube)
        for h in range(sub - 1):
            wide = jnp.where(part == h, value[:, h][..., None], wide)
        spread.append(wide)
    spread = jnp.stack(spread)
    low_bin = jnp.arange(steps, dtype=jnp.int32)[:, None] * sub + part - shift

    def ramp(product):
        angle = jnp.mod(product, cell_count).astype(F32) * (-2.0 * math.pi / cell_count)
        return jnp.stack((jnp.cos(angle), jnp.sin(angle)))

    doppler = jnp.transpose(doppler_phase.reshape(LANES, group_size))
    factor = 1.0 / doppler_phase.shape[0]
    turn = jnp.stack((jnp.cos(doppler) * factor, jnp.sin(doppler) * factor))

    received = []
    source = echoes[0]
    for q in range(sub):
        blocks = []
        for d in range(range_count - 1, 0, -1):
            begin = jnp.mod(place + d, range_count) * n_local + q * piece
            block = lax.dynamic_slice_in_dim(source, begin, piece, 1)
            route = [(i, (i + d) % range_count) for i in range(range_count)]
            blocks.append(lax.ppermute(block, "range", route))
            if d == 1:
                source = lax.optimization_barrier(source)
        received.append(blocks)
    held = echoes[0].reshape(2, range_count, sub, piece, cells_local)
    scalars = jnp.stack((shift, place, below, above))

    twist = ramp((low[:, None] - shift) * (lane[None, :] + cells_local * place))
    samples = []
    gate = None
    for q in range(sub):
        shifts = jnp.tile(pulse_shift[0, q * piece:(q + 1) * piece], sub)
        near = ramp(low_bin * shifts)
        far = ramp(outer * lane[:, None] * shifts)
        gate = twist if gate is None else gate
        first = owned_bins // outer
        data, spill = cells_stage(scalars, held, q, received[q], twist, near, far, spread,
                                  gate, sub, first)
        own = owned_stage(data, near, far, spread, first)
        from_below = shifted(spill, 1)
        from_above = shifted(spill, -1)
        gate = stitch(scalars, own, from_below, from_above, sub,
                      group_size // range_count, range_count)
        blocks = gate.reshape(group_size, bins_local // sub, 2, LANES)
        block = lax.all_to_all(
            blocks, ("range", "pulse"), split_axis=0, concat_axis=0, tiled=True)
        samples.append(jnp.transpose(block, (1, 0, 2, 3)).reshape(
            bins_local // sub, 2 * group_size, LANES))

    early = [spread_stage(samples[q], q, group_size, range_count) for q in range(sub - 1)]
    image = azimuth_stage(early, samples[-1], turn, group_size, range_count)
    image = jnp.transpose(image.reshape(bins_local, group_size, 2, LANES), (0, 2, 1, 3))
    return image.reshape(bins_local, 2, group_size * LANES)


def solution(mesh):
    in_specs = (
        P("band", None, "pulse", "range"),
        P("band", None),
        P("band", ("pulse", "range")),
        P(),
        P(),
    )
    out_specs = P(("band", "pulse", "range"), None, None)
    return jax.shard_map(
        body, mesh=mesh, in_specs=in_specs, out_specs=out_specs, check_vma=False)
```
